256 devices in a mesh: dom: 128 (over z, y, x), st: 2 (over core).
Axes of the slice: x: 4, y: 4, z: 8, core: 2. Of those that a mesh axis runs over, the one named last changes fastest.
Arguments:
- psi: float32 [2, 128, 8, 2, 64, 256], P(None, 'dom', None, None, None, 'st'), parts along dimension 5, may hold values from -18 to 18
- potential: float32 [128, 8, 2, 64], P('dom'), may hold values from 0 to 4
Outputs:
- propagated: float32 [2, 128, 8, 2, 64, 256], P(None, 'dom', None, None, None, 'st'), parts along dimension 5
The draws below stay inside these ranges and needn't reach their ends.
There are 2 independent parts, one for each index of `st`. The reference program is written for one: setup_inputs(seed, part) draws one part's arguments, and reference() takes and returns one part's arrays. A program takes and returns all parts, laid end to end along the dimension named above; an argument that names none is the same for every part. Nothing has to cross between parts.
All inputs are finite; a program needn't handle non-finite values.
Results may differ from the reference program's by a relative error of at most 0.0003.
Values sent between devices are 32-bit elements; how exact they have to be, the bound alone decides.
A program may use at most 64 MiB of HBM per device.

```python
import jax
import jax.numpy as jnp
from jax import lax

CX = 8
BY = 2
NZ = 64
ORB = 128
ITERS = 6
BLOCKS = 128


def draw_psi(key, part):
    shape = (2, BLOCKS, CX, BY, NZ, ORB)
    rising = 1.0 + 2.0 * jnp.arange(BLOCKS, dtype=jnp.float32) / max(BLOCKS - 1, 1)
    rising = rising.reshape(1, BLOCKS, 1, 1, 1, 1)
    return jnp.clip(jax.random.normal(key, shape, jnp.float32), -6.0, 6.0) * rising


def steps_of(rng, dims, shards, smallest, high):
    loudness = 1.0
    for dim, shards_of in shards:
        heights = jax.random.uniform(jax.random.fold_in(jax.random.fold_in(rng, 6), dim), (shards_of,), jnp.float32, smallest / len(shards), high / len(shards))
        loudness = loudness * jnp.repeat(jnp.exp(heights), dims[dim] // shards_of).reshape((-1,) + (1,) * (len(dims) - 1 - dim))
    return loudness


def setup_inputs(seed: int = 0, part: int = 0) -> dict:
    keys = jax.random.split(jax.random.key(seed), 3)
    part_keys = jax.random.split(jax.random.fold_in(keys[2], part), 3)
    psi = draw_psi(jax.random.fold_in(jax.random.fold_in(keys[2], part), 71), part)
    potential = jnp.clip(4.0 * jax.random.uniform(keys[1], (BLOCKS, CX, BY, NZ), jnp.float32) ** steps_of(keys[1], (BLOCKS, CX, BY, NZ), ((0, 128),), -0.2, 0.2), 0.0, 4.0)
    return dict(psi=psi, potential=potential)


epsilon = 1e-06
time_step = 0.5
taylor_terms = 32
far_weight = -1.0 / 12.0
near_weight = 4.0 / 3.0
centre_weight = -7.5

def to_grid(blocked):
    parts, nblocks, cx, by, nz, orbs = blocked.shape
    grid = blocked.transpose(0, 2, 1, 3, 4, 5)
    return grid.reshape(parts, cx, nblocks * by, nz, orbs)

def to_blocks(grid, by):
    parts, nx, ny, nz, orbs = grid.shape
    blocked = grid.reshape(parts, nx, ny // by, by, nz, orbs).transpose(0, 2, 1, 3, 4, 5)
    return blocked

def shift_walls(values, offset):
    width_y = values.shape[2]
    padded = jnp.pad(values, ((0, 0), (0, 0), (2, 2), (0, 0), (0, 0)))
    return padded[:, :, 2 - offset:2 - offset + width_y]

def hamiltonian(values_in, potential):
    total = centre_weight * values_in
    for along in (1, 3):
        total = total + near_weight * (jnp.roll(values_in, 1, along) + jnp.roll(values_in, -1, along))
        total = total + far_weight * (jnp.roll(values_in, 2, along) + jnp.roll(values_in, -2, along))
    total = total + near_weight * (shift_walls(values_in, 1) + shift_walls(values_in, -1))
    total = total + far_weight * (shift_walls(values_in, 2) + shift_walls(values_in, -2))
    return -0.5 * total + potential[None, :, :, :, None] * values_in

def tridiagonal(alphas, betas, vector):
    zero_row = jnp.zeros((1, vector.shape[1]), jnp.float32)
    upper = jnp.concatenate([betas * vector[1:], zero_row], axis=0)
    lower = jnp.concatenate([zero_row, betas * vector[:-1]], axis=0)
    return alphas * vector + upper + lower

def krylov_exponential(alphas, betas):
    count = alphas.shape[0]
    first = (jnp.arange(count) == 0).astype(jnp.float32)[:, None] * jnp.ones_like(alphas)
    term_real = first
    term_imag = jnp.zeros_like(alphas)
    sum_real = term_real
    sum_imag = term_imag
    for order in range(1, taylor_terms):
        applied_real = tridiagonal(alphas, betas, term_real)
        applied_imag = tridiagonal(alphas, betas, term_imag)
        term_real = time_step * applied_imag / order
        term_imag = -time_step * applied_real / order
        sum_real = sum_real + term_real
        sum_imag = sum_imag + term_imag
    return (sum_real, sum_imag)

def reference(psi, potential):
    by = psi.shape[3]
    grid_psi = to_grid(psi)
    grid_pot = to_grid(potential[None, :, :, :, :, None])[0, :, :, :, 0]
    axes_all = (0, 1, 2, 3)
    first_norm = jnp.sqrt(lax.optimization_barrier(jnp.sum(grid_psi * grid_psi, axis=axes_all)) + epsilon)
    vector = grid_psi / first_norm
    previous = jnp.zeros_like(vector)
    beta_prev = jnp.zeros_like(first_norm)
    krylov_basis = []
    alpha_list = []
    beta_list = []
    for iteration in range(ITERS):
        applied = hamiltonian(vector, grid_pot)
        alpha_now = lax.optimization_barrier(jnp.sum(vector * applied, axis=axes_all))
        krylov_basis.append(vector)
        alpha_list.append(alpha_now)
        if iteration + 1 < ITERS:
            remainder = applied - alpha_now * vector - beta_prev * previous
            beta_now = jnp.sqrt(lax.optimization_barrier(jnp.sum(remainder * remainder, axis=axes_all)) + epsilon)
            previous = vector
            vector = remainder / beta_now
            beta_prev = beta_now
            beta_list.append(beta_now)
    coef_real, coef_imag = krylov_exponential(jnp.stack(alpha_list), jnp.stack(beta_list))
    out_real = jnp.zeros_like(grid_psi[0])
    out_imag = jnp.zeros_like(grid_psi[0])
    for index_j in range(ITERS):
        basis_now = krylov_basis[index_j]
        out_real = out_real + coef_real[index_j] * basis_now[0] - coef_imag[index_j] * basis_now[1]
        out_imag = out_imag + coef_real[index_j] * basis_now[1] + coef_imag[index_j] * basis_now[0]
    return to_blocks(first_norm * jnp.stack([out_real, out_imag]), by)
```

```python
import jax
import jax.numpy as jnp
from jax import lax
from jax.experimental import pallas as pl
from jax.experimental.pallas import tpu as pltpu
from jax.sharding import Mesh
from jax.sharding import PartitionSpec as P

MESH = pl.DeviceIdType.MESH
ITERS = 6
TERMS = 32
EPS = 1e-6
STEP = 0.5
SHIFT = 6.0
RADIUS = 6.0
HALO = 6
NX, NY, NZ = 4, 4, 8
PLANE = NX * NY
SLABS = PLANE + 2 * HALO
CHUNKS = 2
OFFSETS = (
    (2, 2), (2, 1), (1, 2), (2, 3), (3, 2), (1, 1), (3, 3), (1, 3), (3, 1),
    (2, 0), (0, 2), (1, 0), (0, 1), (3, 0), (0, 3),
)


def lanczos_weights(moments):
    first_norm = jnp.sqrt(moments[0] + EPS)
    inverse = 1.0 / first_norm
    sig = [value * inverse for value in moments]
    coef = [inverse]
    sig_prev, coef_prev, beta_prev = None, None, None
    alphas, betas, basis = [], [], []
    for j in range(ITERS):
        count = 2 * ITERS - 1 - j
        shifted = [0.5 * RADIUS * (sig[l + 1] + sig[abs(l - 1)]) for l in range(count)]
        alpha = coef[0] * (SHIFT * sig[0] + shifted[0])
        for k in range(1, j + 1):
            alpha = alpha + coef[k] * (SHIFT * sig[k] + shifted[k])
        alpha = jnp.clip(alpha, 0.0, 12.0)
        alphas.append(alpha)
        basis.append(coef)
        if j + 1 == ITERS:
            break
        rest = SHIFT - alpha
        r_sig = [shifted[l] + rest * sig[l] for l in range(count)]
        if j:
            r_sig = [r_sig[l] - beta_prev * sig_prev[l] for l in range(count)]
        r_coef = []
        for k in range(j + 2):
            terms = []
            if k >= 1:
                terms.append((RADIUS if k == 1 else 0.5 * RADIUS) * coef[k - 1])
            if k + 1 <= j:
                terms.append(0.5 * RADIUS * coef[k + 1])
            if k <= j:
                terms.append(rest * coef[k])
            if j and k < j:
                terms.append(-(beta_prev * coef_prev[k]))
            total = terms[0]
            for term in terms[1:]:
                total = total + term
            r_coef.append(total)
        square = r_coef[0] * r_sig[0]
        for k in range(1, j + 2):
            square = square + r_coef[k] * r_sig[k]
        beta = jnp.sqrt(jnp.clip(square, 0.0, 36.5) + EPS)
        betas.append(beta)
        scale = 1.0 / beta
        sig_prev, coef_prev, beta_prev = sig, coef, beta
        sig = [jnp.clip(value * scale, -first_norm, first_norm) for value in r_sig]
        coef = [value * scale for value in r_coef]
    zero = jnp.zeros_like(first_norm)
    term = [zero + 1.0] + [zero] * (ITERS - 1)
    sums = [list(term), [zero] * ITERS]
    for order in range(1, TERMS):
        factor = STEP / order if order % 2 == 0 else -STEP / order
        applied = []
        for i in range(ITERS):
            value = alphas[i] * term[i]
            if i + 1 < ITERS:
                value = value + betas[i] * term[i + 1]
            if i:
                value = value + betas[i - 1] * term[i - 1]
            applied.append(factor * value)
        term = applied
        sums[order % 2] = [a + b for a, b in zip(sums[order % 2], term)]
    weights = []
    for part in range(2):
        row = []
        for k in range(ITERS):
            total = sums[part][k] * basis[k][k]
            for j in range(k + 1, ITERS):
                total = total + sums[part][j] * basis[j][k]
            row.append(first_norm * total)
        weights.append(row)
    return weights


def kernel(psi, pot, out, snd, own_pot, pots, u0, us, outs, back, mixed, gram, *sems):
    (pot_send, pot_recv, pot_halo_send, pot_halo_recv, in_send, in_recv, halo_send, halo_recv,
     gram_send, gram_recv, out_send, out_recv) = sems
    z, y, x, st = (lax.axis_index(name) for name in ("dom_0", "dom_1", "dom_2", "st"))
    me = y * NX + x
    lane = lax.broadcasted_iota(jnp.int32, (8, 128), 1)
    sub = lax.broadcasted_iota(jnp.int32, (8, 128), 0)

    def at(offset):
        to_y = lax.rem(y + offset[0], NY)
        to_x = lax.rem(x + offset[1], NX)
        return to_y * NX + to_x, (z, to_y, to_x, st)

    barrier = pltpu.get_barrier_semaphore()
    for offset in OFFSETS:
        pl.semaphore_signal(barrier, inc=1, device_id=at(offset)[1], device_id_type=MESH)
    for dz in range(1, NZ):
        pl.semaphore_signal(barrier, inc=1, device_id=(lax.rem(z + dz, NZ), y, x, st), device_id_type=MESH)

    for j in range(2):
        tile = jnp.concatenate([pot[0:4, j, :], pot[4:8, j, :]], axis=1)
        own_pot[4 * j : 4 * j + 4, :] = tile
    pots[HALO + me] = own_pot[...]

    wide = lax.broadcasted_iota(jnp.int32, (128, 128), 1)
    low = lax.rem(wide, 8) < 4

    def to_peers(chunk):
        for j in range(2):
            for i in range(4):
                re = jnp.concatenate([psi[0, i, j], psi[0, i + 4, j]], axis=0)
                im = jnp.concatenate([psi[1, i, j], psi[1, i + 4, j]], axis=0)
                if chunk == 0:
                    both = jnp.where(low, re, pltpu.roll(im, 4, 1))
                else:
                    both = jnp.where(low, pltpu.roll(re, 124, 1), im)
                snd[chunk, :, j, i] = both.T.reshape(PLANE, 8, 128)

    def send_in(chunk):
        for number, offset in enumerate(OFFSETS):
            peer, where = at(offset)
            pltpu.make_async_remote_copy(
                src_ref=snd.at[chunk, peer], dst_ref=u0.at[chunk, HALO + me],
                send_sem=in_send.at[chunk, number], recv_sem=in_recv.at[chunk, me],
                device_id=where, device_id_type=MESH,
            ).start()

    to_peers(0)
    pl.semaphore_wait(barrier, len(OFFSETS) + NZ - 1)
    for number, offset in enumerate(OFFSETS):
        peer, where = at(offset)
        pltpu.make_async_remote_copy(
            src_ref=own_pot, dst_ref=pots.at[HALO + me],
            send_sem=pot_send.at[number], recv_sem=pot_recv.at[me],
            device_id=where, device_id_type=MESH,
        ).start()
    send_in(0)
    to_peers(1)
    send_in(1)
    for chunk in range(CHUNKS):
        u0[chunk, HALO + me] = snd[chunk, me]

    has_low, has_high = z > 0, z < NZ - 1
    below, above = (jnp.maximum(z - 1, 0), y, x, st), (jnp.minimum(z + 1, NZ - 1), y, x, st)

    @pl.when(jnp.logical_not(has_low))
    def _():
        for chunk in range(CHUNKS):
            u0[chunk, 0:HALO] = jnp.zeros((HALO,) + u0.shape[2:], jnp.float32)
        pots[0:HALO] = jnp.zeros((HALO, 8, 128), jnp.float32)

    @pl.when(jnp.logical_not(has_high))
    def _():
        for chunk in range(CHUNKS):
            u0[chunk, HALO + PLANE : SLABS] = jnp.zeros((HALO,) + u0.shape[2:], jnp.float32)
        pots[HALO + PLANE : SLABS] = jnp.zeros((HALO, 8, 128), jnp.float32)

    def wait_recv(ref, sem):
        pltpu.make_async_remote_copy(
            src_ref=ref, dst_ref=ref, send_sem=sem, recv_sem=sem,
            device_id=(z, y, x, st), device_id_type=MESH,
        ).wait_recv()

    def wait_send(ref, sem):
        pltpu.make_async_remote_copy(
            src_ref=ref, dst_ref=ref, send_sem=sem, recv_sem=sem,
            device_id=(z, y, x, st), device_id_type=MESH,
        ).wait_send()

    def halo_copy(chunk, slot, up):
        source = PLANE + slot if up else HALO + slot
        target = slot if up else HALO + PLANE + slot
        return pltpu.make_async_remote_copy(
            src_ref=u0.at[chunk, source], dst_ref=u0.at[chunk, target],
            send_sem=halo_send.at[chunk, int(up), slot], recv_sem=halo_recv.at[chunk, int(up), slot],
            device_id=above if up else below, device_id_type=MESH,
        )

    def pot_halo_copy(up):
        source = PLANE if up else HALO
        target = 0 if up else HALO + PLANE
        return pltpu.make_async_remote_copy(
            src_ref=pots.at[pl.ds(source, HALO)], dst_ref=pots.at[pl.ds(target, HALO)],
            send_sem=pot_halo_send.at[int(up)], recv_sem=pot_halo_recv.at[int(up)],
            device_id=above if up else below, device_id_type=MESH,
        )

    def forward(chunk):
        for p in range(PLANE):
            @pl.when(me != p)
            def _():
                wait_recv(u0.at[chunk, HALO + p], in_recv.at[chunk, p])
            if p < HALO:
                @pl.when(has_low)
                def _():
                    halo_copy(chunk, p, False).start()
            if p >= PLANE - HALO:
                @pl.when(has_high)
                def _():
                    halo_copy(chunk, p - PLANE + HALO, True).start()

    for p in range(PLANE):
        @pl.when(me != p)
        def _():
            wait_recv(pots.at[HALO + p], pot_recv.at[p])

    @pl.when(has_low)
    def _():
        pot_halo_copy(False).start()

    @pl.when(has_high)
    def _():
        pot_halo_copy(True).start()

    for chunk in range(CHUNKS):
        forward(chunk)

    @pl.when(has_low)
    def _():
        pot_halo_copy(True).wait_recv()

    @pl.when(has_high)
    def _():
        pot_halo_copy(False).wait_recv()

    low_mask = jnp.where(has_low, 1.0, 0.0)
    high_mask = jnp.where(has_high, 1.0, 0.0)
    half = lane & 64
    spot = lane & 63
    shifts = [half | ((spot + d) & 63) for d in (-1, 1, -2, 2)]

    def pick(value, index):
        return jnp.take_along_axis(value, index, axis=1, mode="promise_in_bounds")

    centre = (3.75 - SHIFT) * (2.0 / RADIUS)
    near_w = -(2.0 / 3.0) * (2.0 / RADIUS)
    far_w = (1.0 / 24.0) * (2.0 / RADIUS)

    def apply(chunk, k, b, mask):
        size = 0.5 if k == 0 else 1.0
        source = (lambda s, j, i: u0[chunk, s, j, i]) if k == 0 else (lambda s, j, i: us[chunk, k - 1, s, j, i])
        before = [[source(b - 1, j, i) for i in range(4)] for j in range(2)]
        here = [[source(b, j, i) for i in range(4)] for j in range(2)]
        after = [[source(b + 1, j, i) for i in range(4)] for j in range(2)]
        rows = [before[0], before[1], here[0], here[1], after[0], after[1]]
        values, results = [], []
        for j in range(2):
            row = rows[2 + j]
            swap = [pltpu.roll(v, 64, 1) for v in row]
            ring = [swap[2], swap[3]] + row + [swap[0], swap[1]]
            for i in range(4):
                v = row[i]
                zs = [pick(v, index) for index in shifts]
                near = (ring[i + 1] + ring[i + 3]) + (rows[1 + j][i] + rows[3 + j][i]) + (zs[0] + zs[1])
                far = (ring[i] + ring[i + 4]) + (rows[j][i] + rows[4 + j][i]) + (zs[2] + zs[3])
                weight = (2.0 / RADIUS * size) * pots[b, pl.ds(4 * j + i, 1), :] + centre * size
                new = weight * v + ((near_w * size) * near + (far_w * size) * far)
                if k == 1:
                    new = new - u0[chunk, b, j, i]
                elif k > 1:
                    new = new - us[chunk, k - 2, b, j, i]
                if mask is not None:
                    new = new * mask
                values.append(v)
                results.append(new)
                if k + 1 < ITERS:
                    us[chunk, k, b, j, i] = new
        return values, results

    def tree(values):
        while len(values) > 1:
            values = [values[i] + values[i + 1] for i in range(0, len(values) - 1, 2)] + (
                [values[-1]] if len(values) % 2 else []
            )
        return values[0]

    zero = jnp.zeros((8, 128), jnp.float32)

    def moments_of(chunk):
        pairs = []
        for k in range(ITERS):
            def low_body(b, carry):
                apply(chunk, k, b, low_mask)
                return carry

            def high_body(b, carry):
                apply(chunk, k, b, high_mask)
                return carry

            def own_body(b, carry):
                values, results = apply(chunk, k, b, None)
                same = tree([v * v for v in values])
                next_ = tree([v * r for v, r in zip(values, results)])
                return carry[0] + same, carry[1] + next_

            if k + 1 < ITERS:
                lax.fori_loop(1 + k, HALO, low_body, 0)
                lax.fori_loop(HALO + PLANE, SLABS - 1 - k, high_body, 0)
            pairs.append(lax.fori_loop(HALO, HALO + PLANE, own_body, (zero, zero)))
        tile = zero
        for k, pair in enumerate(pairs):
            for odd in range(2):
                total = jnp.sum(pair[odd], axis=1, keepdims=True)
                tile = jnp.where(lane == 2 * k + odd, total, tile)
        return tile

    def send_gram(chunk):
        for dz in range(1, NZ):
            pltpu.make_async_remote_copy(
                src_ref=gram.at[chunk, z], dst_ref=gram.at[chunk, z],
                send_sem=gram_send.at[chunk, dz], recv_sem=gram_recv.at[chunk, z],
                device_id=(lax.rem(z + dz, NZ), y, x, st), device_id_type=MESH,
            ).start()

    for chunk in range(CHUNKS):
        for slot in range(HALO):
            @pl.when(has_low)
            def _():
                halo_copy(chunk, slot, True).wait_recv()

            @pl.when(has_high)
            def _():
                halo_copy(chunk, slot, False).wait_recv()
        gram[chunk, z] = moments_of(chunk)
        send_gram(chunk)

    def finish(chunk):
        for p in range(NZ):
            @pl.when(z != p)
            def _():
                wait_recv(gram.at[chunk, p], gram_recv.at[chunk, p])
        total = tree([gram[chunk, p] for p in range(NZ)])
        total = total + pltpu.roll(total, 4, 0)
        raw = [jnp.broadcast_to(total[:, l : l + 1], (8, 128)) for l in range(2 * ITERS)]
        moments = raw[:2] + [2.0 * raw[l] - raw[l % 2] for l in range(2, 2 * ITERS)]
        real, imag = lanczos_weights(moments)
        imag = [jnp.where(sub < 4, value, -value) for value in imag]

        def combine(q, carry):
            for j in range(2):
                for i in range(4):
                    v = u0[chunk, HALO + q, j, i]
                    straight, crossed = real[0] * v, imag[0] * v
                    for k in range(1, ITERS):
                        v = us[chunk, k - 1, HALO + q, j, i]
                        straight = straight + real[k] * v
                        crossed = crossed + imag[k] * v
                    outs[chunk, q, j, i] = straight + pltpu.roll(crossed, 4, 0)
            return carry

        lax.fori_loop(0, PLANE, combine, 0)
        for number, offset in enumerate(OFFSETS):
            peer, where = at(offset)
            pltpu.make_async_remote_copy(
                src_ref=outs.at[chunk, peer], dst_ref=back.at[chunk, me],
                send_sem=out_send.at[chunk, number], recv_sem=out_recv.at[chunk, me],
                device_id=where, device_id_type=MESH,
            ).start()
        back[chunk, me] = outs[chunk, me]

    for chunk in range(CHUNKS):
        finish(chunk)

    for chunk in range(CHUNKS):
        for p in range(PLANE):
            @pl.when(me != p)
            def _():
                wait_recv(back.at[chunk, p], out_recv.at[chunk, p])
        for j in range(2):
            for i in range(4):
                cells = back[chunk, :, j, i].reshape(128, 128).T
                if chunk == 0:
                    mixed[j, i] = cells
                else:
                    first = mixed[j, i]
                    re = jnp.where(low, first, pltpu.roll(cells, 4, 1))
                    im = jnp.where(low, pltpu.roll(first, 124, 1), cells)
                    out[0, i, j] = re[0:64]
                    out[0, i + 4, j] = re[64:128]
                    out[1, i, j] = im[0:64]
                    out[1, i + 4, j] = im[64:128]

    for number in range(len(OFFSETS)):
        wait_send(own_pot, pot_send.at[number])
        for chunk in range(CHUNKS):
            wait_send(snd.at[chunk, 0], in_send.at[chunk, number])
            wait_send(outs.at[chunk, 0], out_send.at[chunk, number])
    for chunk in range(CHUNKS):
        for dz in range(1, NZ):
            wait_send(gram.at[chunk, 0], gram_send.at[chunk, dz])

    @pl.when(has_low)
    def _():
        pot_halo_copy(False).wait_send()
        for chunk in range(CHUNKS):
            for slot in range(HALO):
                halo_copy(chunk, slot, False).wait_send()

    @pl.when(has_high)
    def _():
        pot_halo_copy(True).wait_send()
        for chunk in range(CHUNKS):
            for slot in range(HALO):
                halo_copy(chunk, slot, True).wait_send()


def on_device(psi, potential):
    parts, _, cx, by, nz, orbs = psi.shape
    dma = pltpu.SemaphoreType.DMA
    peers = len(OFFSETS)
    tiles = (2, 4, 8, 128)
    result = pl.pallas_call(
        kernel,
        out_shape=jax.ShapeDtypeStruct((parts, cx, by, nz, orbs), jnp.float32),
        in_specs=[pl.BlockSpec(memory_space=pltpu.VMEM)] * 2,
        out_specs=pl.BlockSpec(memory_space=pltpu.VMEM),
        scratch_shapes=[
            pltpu.VMEM((CHUNKS, PLANE) + tiles, jnp.float32),
            pltpu.VMEM((8, 128), jnp.float32),
            pltpu.VMEM((SLABS, 8, 128), jnp.float32),
            pltpu.VMEM((CHUNKS, SLABS) + tiles, jnp.float32),
            pltpu.VMEM((CHUNKS, ITERS - 1, SLABS) + tiles, jnp.float32),
            pltpu.VMEM((CHUNKS, PLANE) + tiles, jnp.float32),
            pltpu.VMEM((CHUNKS, PLANE) + tiles, jnp.float32),
            pltpu.VMEM((2, 4, 128, 128), jnp.float32),
            pltpu.VMEM((CHUNKS, NZ, 8, 128), jnp.float32),
            dma((peers,)), dma((PLANE,)), dma((2,)), dma((2,)),
            dma((CHUNKS, peers)), dma((CHUNKS, PLANE)),
            dma((CHUNKS, 2, HALO)), dma((CHUNKS, 2, HALO)),
            dma((CHUNKS, NZ)), dma((CHUNKS, NZ)),
            dma((CHUNKS, peers)), dma((CHUNKS, PLANE)),
        ],
        compiler_params=pltpu.CompilerParams(
            collective_id=0, has_side_effects=True, vmem_limit_bytes=48 * 1024 * 1024
        ),
    )(psi.reshape(parts, cx, by, nz, orbs), potential.reshape(cx, by, nz))
    return result.reshape(psi.shape)


def solution(mesh):
    names = ("dom_0", "dom_1", "dom_2", "st")
    torus = Mesh(mesh.devices.reshape(NZ, NY, NX, mesh.shape["st"]), names)
    placed = (P(None, names[:3], None, None, None, "st"), P(names[:3], None, None, None))
    return jax.shard_map(
        on_device,
        mesh=torus,
        in_specs=placed,
        out_specs=P(None, names[:3], None, None, None, "st"),
        check_vma=False,
    )
```

```python
import jax
import jax.numpy as jnp
from jax import lax
from jax.experimental import pallas as pl
from jax.experimental.pallas import tpu as pltpu
from jax.sharding import Mesh
from jax.sharding import PartitionSpec as P

MESH = pl.DeviceIdType.MESH
ITERS = 6
TERMS = 32
EPS = 1e-6
STEP = 0.5
SHIFT = 6.0
RADIUS = 6.0
HALO = 6
NX, NY, NZ = 4, 4, 8
PLANE = NX * NY
SLABS = PLANE + 2 * HALO
CHUNKS = 2
GROUP = 4
OFFSETS = (
    (2, 2), (2, 1), (1, 2), (2, 3), (3, 2), (1, 1), (3, 3), (1, 3), (3, 1),
    (2, 0), (0, 2), (1, 0), (0, 1), (3, 0), (0, 3),
)


def lanczos_weights(moments):
    first_norm = jnp.sqrt(moments[0] + EPS)
    inverse = 1.0 / first_norm
    sig = [value * inverse for value in moments]
    coef = [inverse]
    sig_prev, coef_prev, beta_prev = None, None, None
    alphas, betas, basis = [], [], []
    for j in range(ITERS):
        count = 2 * ITERS - 1 - j
        shifted = [0.5 * RADIUS * (sig[l + 1] + sig[abs(l - 1)]) for l in range(count)]
        alpha = coef[0] * (SHIFT * sig[0] + shifted[0])
        for k in range(1, j + 1):
            alpha = alpha + coef[k] * (SHIFT * sig[k] + shifted[k])
        alpha = jnp.clip(alpha, 0.0, 12.0)
        alphas.append(alpha)
        basis.append(coef)
        if j + 1 == ITERS:
            break
        rest = SHIFT - alpha
        r_sig = [shifted[l] + rest * sig[l] for l in range(count)]
        if j:
            r_sig = [r_sig[l] - beta_prev * sig_prev[l] for l in range(count)]
        r_coef = []
        for k in range(j + 2):
            terms = []
            if k >= 1:
                terms.append((RADIUS if k == 1 else 0.5 * RADIUS) * coef[k - 1])
            if k + 1 <= j:
                terms.append(0.5 * RADIUS * coef[k + 1])
            if k <= j:
                terms.append(rest * coef[k])
            if j and k < j:
                terms.append(-(beta_prev * coef_prev[k]))
            total = terms[0]
            for term in terms[1:]:
                total = total + term
            r_coef.append(total)
        square = r_coef[0] * r_sig[0]
        for k in range(1, j + 2):
            square = square + r_coef[k] * r_sig[k]
        beta = jnp.sqrt(jnp.clip(square, 0.0, 36.5) + EPS)
        betas.append(beta)
        scale = 1.0 / beta
        sig_prev, coef_prev, beta_prev = sig, coef, beta
        sig = [jnp.clip(value * scale, -first_norm, first_norm) for value in r_sig]
        coef = [value * scale for value in r_coef]
    zero = jnp.zeros_like(first_norm)
    term = [zero + 1.0] + [zero] * (ITERS - 1)
    sums = [list(term), [zero] * ITERS]
    for order in range(1, TERMS):
        factor = STEP / order if order % 2 == 0 else -STEP / order
        applied = []
        for i in range(ITERS):
            value = alphas[i] * term[i]
            if i + 1 < ITERS:
                value = value + betas[i] * term[i + 1]
            if i:
                value = value + betas[i - 1] * term[i - 1]
            applied.append(factor * value)
        term = applied
        sums[order % 2] = [a + b for a, b in zip(sums[order % 2], term)]
    weights = []
    for part in range(2):
        row = []
        for k in range(ITERS):
            total = sums[part][k] * basis[k][k]
            for j in range(k + 1, ITERS):
                total = total + sums[part][j] * basis[j][k]
            row.append(first_norm * total)
        weights.append(row)
    return weights


def kernel(psi_hbm, pot, out, psi, snd, own_pot, pots, centre, u0, u1, u2, u3, u4, u5, crossed_z, matrix, outs, back, mixed, gram, *sems):
    us = (u1, u2, u3, u4, u5)
    (psi_in, pot_send, pot_recv, pot_halo_send, pot_halo_recv, in_send, in_recv, halo_send, halo_recv,
     gram_send, gram_recv, out_send, out_recv) = sems
    z, y, x, st = (lax.axis_index(name) for name in ("dom_0", "dom_1", "dom_2", "st"))
    me = y * NX + x
    lane = lax.broadcasted_iota(jnp.int32, (8, 128), 1)
    sub = lax.broadcasted_iota(jnp.int32, (8, 128), 0)

    def at(offset):
        to_y = lax.rem(y + offset[0], NY)
        to_x = lax.rem(x + offset[1], NX)
        return to_y * NX + to_x, (z, to_y, to_x, st)

    barrier = pltpu.get_barrier_semaphore()
    for offset in OFFSETS:
        pl.semaphore_signal(barrier, inc=1, device_id=at(offset)[1], device_id_type=MESH)
    for dz in range(1, NZ):
        pl.semaphore_signal(barrier, inc=1, device_id=(lax.rem(z + dz, NZ), y, x, st), device_id_type=MESH)

    load = pltpu.make_async_copy(psi_hbm, psi, psi_in)
    load.start()

    from_lane = lax.broadcasted_iota(jnp.int32, (128, 128), 0)
    to_lane = lax.broadcasted_iota(jnp.int32, (128, 128), 1)
    apart = (from_lane - to_lane) & 63
    together = (from_lane & 64) == (to_lane & 64)
    along_z = jnp.where((apart == 1) | (apart == 63), 16.0, jnp.where((apart == 2) | (apart == 62), -1.0, 0.0))
    along_z = jnp.where(together, along_z, 0.0)
    swapped = jnp.where((from_lane ^ 64) == to_lane, 1.0, 0.0)
    for piece in range(2):
        matrix[128 * piece : 128 * piece + 128, 0:128] = along_z.astype(jnp.bfloat16)
        matrix[128 * piece : 128 * piece + 128, 128:256] = swapped.astype(jnp.bfloat16)

    for j in range(2):
        tile = jnp.concatenate([pot[0:4, j, :], pot[4:8, j, :]], axis=1)
        own_pot[4 * j : 4 * j + 4, :] = tile
    pots[HALO + me] = own_pot[...]

    wide = lax.broadcasted_iota(jnp.int32, (128, 128), 1)
    low = lax.rem(wide, 8) < 4

    def to_peers(chunk):
        for j in range(2):
            for i in range(4):
                re = jnp.concatenate([psi[0, i, j], psi[0, i + 4, j]], axis=0)
                im = jnp.concatenate([psi[1, i, j], psi[1, i + 4, j]], axis=0)
                if chunk == 0:
                    both = jnp.where(low, re, pltpu.roll(im, 4, 1))
                else:
                    both = jnp.where(low, pltpu.roll(re, 124, 1), im)
                snd[chunk, :, j, i] = both.T.reshape(PLANE, 8, 128)

    def send_in(chunk):
        for number, offset in enumerate(OFFSETS):
            peer, where = at(offset)
            pltpu.make_async_remote_copy(
                src_ref=snd.at[chunk, peer], dst_ref=u0.at[chunk, HALO + me],
                send_sem=in_send.at[chunk, number], recv_sem=in_recv.at[chunk, me],
                device_id=where, device_id_type=MESH,
            ).start()

    load.wait()
    to_peers(0)
    pl.semaphore_wait(barrier, len(OFFSETS) + NZ - 1)
    for number, offset in enumerate(OFFSETS):
        peer, where = at(offset)
        pltpu.make_async_remote_copy(
            src_ref=own_pot, dst_ref=pots.at[HALO + me],
            send_sem=pot_send.at[number], recv_sem=pot_recv.at[me],
            device_id=where, device_id_type=MESH,
        ).start()
    send_in(0)
    to_peers(1)
    send_in(1)
    for chunk in range(CHUNKS):
        u0[chunk, HALO + me] = snd[chunk, me]

    has_low, has_high = z > 0, z < NZ - 1
    below, above = (jnp.maximum(z - 1, 0), y, x, st), (jnp.minimum(z + 1, NZ - 1), y, x, st)

    @pl.when(jnp.logical_not(has_low))
    def _():
        for chunk in range(CHUNKS):
            u0[chunk, 0:HALO] = jnp.zeros((HALO,) + u0.shape[2:], jnp.float32)
        pots[0:HALO] = jnp.zeros((HALO, 8, 128), jnp.float32)

    @pl.when(jnp.logical_not(has_high))
    def _():
        for chunk in range(CHUNKS):
            u0[chunk, HALO + PLANE : SLABS] = jnp.zeros((HALO,) + u0.shape[2:], jnp.float32)
        pots[HALO + PLANE : SLABS] = jnp.zeros((HALO, 8, 128), jnp.float32)

    def wait_recv(ref, sem):
        pltpu.make_async_remote_copy(
            src_ref=ref, dst_ref=ref, send_sem=sem, recv_sem=sem,
            device_id=(z, y, x, st), device_id_type=MESH,
        ).wait_recv()

    def wait_send(ref, sem):
        pltpu.make_async_remote_copy(
            src_ref=ref, dst_ref=ref, send_sem=sem, recv_sem=sem,
            device_id=(z, y, x, st), device_id_type=MESH,
        ).wait_send()

    def halo_copy(chunk, slot, up):
        source = PLANE + slot if up else HALO + slot
        target = slot if up else HALO + PLANE + slot
        return pltpu.make_async_remote_copy(
            src_ref=u0.at[chunk, source], dst_ref=u0.at[chunk, target],
            send_sem=halo_send.at[chunk, int(up), slot], recv_sem=halo_recv.at[chunk, int(up), slot],
            device_id=above if up else below, device_id_type=MESH,
        )

    def pot_halo_copy(up):
        source = PLANE if up else HALO
        target = 0 if up else HALO + PLANE
        return pltpu.make_async_remote_copy(
            src_ref=pots.at[pl.ds(source, HALO)], dst_ref=pots.at[pl.ds(target, HALO)],
            send_sem=pot_halo_send.at[int(up)], recv_sem=pot_halo_recv.at[int(up)],
            device_id=above if up else below, device_id_type=MESH,
        )

    def forward(chunk):
        for p in range(PLANE):
            @pl.when(me != p)
            def _():
                wait_recv(u0.at[chunk, HALO + p], in_recv.at[chunk, p])
            if p < HALO:
                @pl.when(has_low)
                def _():
                    halo_copy(chunk, p, False).start()
            if p >= PLANE - HALO:
                @pl.when(has_high)
                def _():
                    halo_copy(chunk, p - PLANE + HALO, True).start()

    for p in range(PLANE):
        @pl.when(me != p)
        def _():
            wait_recv(pots.at[HALO + p], pot_recv.at[p])

    @pl.when(has_low)
    def _():
        pot_halo_copy(False).start()

    @pl.when(has_high)
    def _():
        pot_halo_copy(True).start()

    for chunk in range(CHUNKS):
        forward(chunk)

    @pl.when(has_low)
    def _():
        pot_halo_copy(True).wait_recv()

    @pl.when(has_high)
    def _():
        pot_halo_copy(False).wait_recv()

    low_mask = jnp.where(has_low, 1.0, 0.0)
    high_mask = jnp.where(has_high, 1.0, 0.0)
    centre[...] = (2.0 / RADIUS) * pots[...] + (3.75 - SHIFT) * (2.0 / RADIUS)
    far_w = (1.0 / 24.0) * (2.0 / RADIUS)

    def source(k):
        return us[k - 1] if k else u0

    def cross(chunk, k, first, count):
        value = source(k)[chunk, first : first + count].reshape(count * 64, 128)
        top = value.astype(jnp.bfloat16)
        rest = (value - top.astype(jnp.float32)).astype(jnp.bfloat16)
        crossed_z[first * 64 : (first + count) * 64, :] = jnp.dot(
            jnp.concatenate([top, rest], axis=1), matrix[...], preferred_element_type=jnp.float32
        )

    def apply(chunk, k, b, mask):
        u = source(k)
        rows = [[u[chunk, b + s, j, i] for i in range(4)] for s in (-1, 0, 1) for j in range(2)]
        values, results = [], []
        for j in range(2):
            row = rows[2 + j]
            start = b * 64 + j * 32
            swap = [crossed_z[start + 8 * i : start + 8 * i + 8, 128:256] for i in range(4)]
            ring = [swap[2], swap[3]] + row + [swap[0], swap[1]]
            for i in range(4):
                v = row[i]
                near = (ring[i + 1] + ring[i + 3]) + (rows[1 + j][i] + rows[3 + j][i])
                far = (ring[i] + ring[i + 4]) + (rows[j][i] + rows[4 + j][i])
                total = (16.0 * near - far) + crossed_z[start + 8 * i : start + 8 * i + 8, 0:128]
                new = centre[b, pl.ds(4 * j + i, 1), :] * v - far_w * total
                if k == 0:
                    new = 0.5 * new
                else:
                    new = new - source(k - 1)[chunk, b, j, i]
                if mask is not None:
                    new = new * mask
                values.append(v)
                results.append(new)
                if k + 1 < ITERS:
                    us[k][chunk, b, j, i] = new
        return values, results

    def tree(values):
        while len(values) > 1:
            values = [values[i] + values[i + 1] for i in range(0, len(values) - 1, 2)] + (
                [values[-1]] if len(values) % 2 else []
            )
        return values[0]

    zero = jnp.zeros((8, 128), jnp.float32)

    def moments_of(chunk):
        pairs = []
        for k in range(ITERS):
            first, last = 1 + k, SLABS - 1 - k
            groups = [(at_, min(GROUP, last - at_)) for at_ in range(first, last, GROUP)]
            same, next_ = zero, zero
            cross(chunk, k, *groups[0])
            for number, (start, count) in enumerate(groups):
                if number + 1 < len(groups):
                    cross(chunk, k, *groups[number + 1])
                for b in range(start, start + count):
                    mine = HALO <= b < HALO + PLANE
                    mask = None if mine else (low_mask if b < HALO else high_mask)
                    values, results = apply(chunk, k, b, mask)
                    if mine:
                        same = same + tree([v * v for v in values])
                        next_ = next_ + tree([v * r for v, r in zip(values, results)])
            pairs.append((same, next_))
        tile = zero
        for k, pair in enumerate(pairs):
            for odd in range(2):
                total = jnp.sum(pair[odd], axis=1, keepdims=True)
                tile = jnp.where(lane == 2 * k + odd, total, tile)
        return tile

    def send_gram(chunk):
        for dz in range(1, NZ):
            pltpu.make_async_remote_copy(
                src_ref=gram.at[chunk, z], dst_ref=gram.at[chunk, z],
                send_sem=gram_send.at[chunk, dz], recv_sem=gram_recv.at[chunk, z],
                device_id=(lax.rem(z + dz, NZ), y, x, st), device_id_type=MESH,
            ).start()

    def advance(chunk, carry):
        for slot in range(HALO):
            @pl.when(has_low)
            def _():
                halo_copy(chunk, slot, True).wait_recv()

            @pl.when(has_high)
            def _():
                halo_copy(chunk, slot, False).wait_recv()
        gram[chunk, z] = moments_of(chunk)
        send_gram(chunk)
        return carry

    lax.fori_loop(0, CHUNKS, advance, 0)

    def finish(chunk):
        for p in range(NZ):
            @pl.when(z != p)
            def _():
                wait_recv(gram.at[chunk, p], gram_recv.at[chunk, p])
        total = tree([gram[chunk, p] for p in range(NZ)])
        total = total + pltpu.roll(total, 4, 0)
        raw = [jnp.broadcast_to(total[:, l : l + 1], (8, 128)) for l in range(2 * ITERS)]
        moments = raw[:2] + [2.0 * raw[l] - raw[l % 2] for l in range(2, 2 * ITERS)]
        real, imag = lanczos_weights(moments)
        imag = [jnp.where(sub < 4, value, -value) for value in imag]

        def combine(q, carry):
            for j in range(2):
                for i in range(4):
                    v = u0[chunk, HALO + q, j, i]
                    straight, crossed = real[0] * v, imag[0] * v
                    for k in range(1, ITERS):
                        v = us[k - 1][chunk, HALO + q, j, i]
                        straight = straight + real[k] * v
                        crossed = crossed + imag[k] * v
                    outs[chunk, q, j, i] = straight + pltpu.roll(crossed, 4, 0)
            return carry

        lax.fori_loop(0, PLANE, combine, 0)
        for number, offset in enumerate(OFFSETS):
            peer, where = at(offset)
            pltpu.make_async_remote_copy(
                src_ref=outs.at[chunk, peer], dst_ref=back.at[chunk, me],
                send_sem=out_send.at[chunk, number], recv_sem=out_recv.at[chunk, me],
                device_id=where, device_id_type=MESH,
            ).start()
        back[chunk, me] = outs[chunk, me]

    for chunk in range(CHUNKS):
        finish(chunk)

    for chunk in range(CHUNKS):
        for p in range(PLANE):
            @pl.when(me != p)
            def _():
                wait_recv(back.at[chunk, p], out_recv.at[chunk, p])
        for j in range(2):
            for i in range(4):
                cells = back[chunk, :, j, i].reshape(128, 128).T
                if chunk == 0:
                    mixed[j, i] = cells
                else:
                    first = mixed[j, i]
                    re = jnp.where(low, first, pltpu.roll(cells, 4, 1))
                    im = jnp.where(low, pltpu.roll(first, 124, 1), cells)
                    out[0, i, j] = re[0:64]
                    out[0, i + 4, j] = re[64:128]
                    out[1, i, j] = im[0:64]
                    out[1, i + 4, j] = im[64:128]

    for number in range(len(OFFSETS)):
        wait_send(own_pot, pot_send.at[number])
        for chunk in range(CHUNKS):
            wait_send(snd.at[chunk, 0], in_send.at[chunk, number])
            wait_send(outs.at[chunk, 0], out_send.at[chunk, number])
    for chunk in range(CHUNKS):
        for dz in range(1, NZ):
            wait_send(gram.at[chunk, 0], gram_send.at[chunk, dz])

    @pl.when(has_low)
    def _():
        pot_halo_copy(False).wait_send()
        for chunk in range(CHUNKS):
            for slot in range(HALO):
                halo_copy(chunk, slot, False).wait_send()

    @pl.when(has_high)
    def _():
        pot_halo_copy(True).wait_send()
        for chunk in range(CHUNKS):
            for slot in range(HALO):
                halo_copy(chunk, slot, True).wait_send()


def on_device(psi, potential):
    parts, _, cx, by, nz, orbs = psi.shape
    dma = pltpu.SemaphoreType.DMA
    peers = len(OFFSETS)
    tiles = (2, 4, 8, 128)
    result = pl.pallas_call(
        kernel,
        out_shape=jax.ShapeDtypeStruct((parts, cx, by, nz, orbs), jnp.float32),
        in_specs=[pl.BlockSpec(memory_space=pl.ANY), pl.BlockSpec(memory_space=pltpu.VMEM)],
        out_specs=pl.BlockSpec(memory_space=pltpu.VMEM),
        scratch_shapes=[
            pltpu.VMEM((parts, cx, by, nz, orbs), jnp.float32),
            pltpu.VMEM((CHUNKS, PLANE) + tiles, jnp.float32),
            pltpu.VMEM((8, 128), jnp.float32),
            pltpu.VMEM((SLABS, 8, 128), jnp.float32),
            pltpu.VMEM((SLABS, 8, 128), jnp.float32),
            *[pltpu.VMEM((CHUNKS, SLABS) + tiles, jnp.float32)] * ITERS,
            pltpu.VMEM((SLABS * 64, 256), jnp.float32),
            pltpu.VMEM((256, 256), jnp.bfloat16),
            pltpu.VMEM((CHUNKS, PLANE) + tiles, jnp.float32),
            pltpu.VMEM((CHUNKS, PLANE) + tiles, jnp.float32),
            pltpu.VMEM((2, 4, 128, 128), jnp.float32),
            pltpu.VMEM((CHUNKS, NZ, 8, 128), jnp.float32),
            dma, dma((peers,)), dma((PLANE,)), dma((2,)), dma((2,)),
            dma((CHUNKS, peers)), dma((CHUNKS, PLANE)),
            dma((CHUNKS, 2, HALO)), dma((CHUNKS, 2, HALO)),
            dma((CHUNKS, NZ)), dma((CHUNKS, NZ)),
            dma((CHUNKS, peers)), dma((CHUNKS, PLANE)),
        ],
        compiler_params=pltpu.CompilerParams(
            collective_id=0, has_side_effects=True, vmem_limit_bytes=67043328
        ),
    )(psi.reshape(parts, cx, by, nz, orbs), potential.reshape(cx, by, nz))
    return result.reshape(psi.shape)


def solution(mesh):
    names = ("dom_0", "dom_1", "dom_2", "st")
    torus = Mesh(mesh.devices.reshape(NZ, NY, NX, mesh.shape["st"]), names)
    placed = (P(None, names[:3], None, None, None, "st"), P(names[:3], None, None, None))
    return jax.shard_map(
        on_device,
        mesh=torus,
        in_specs=placed,
        out_specs=P(None, names[:3], None, None, None, "st"),
        check_vma=False,
    )
```

```python
import jax
import jax.numpy as jnp
from jax import lax
from jax.experimental import pallas as pl
from jax.experimental.pallas import tpu as pltpu
from jax.sharding import Mesh
from jax.sharding import PartitionSpec as P

MESH = pl.DeviceIdType.MESH
ITERS = 6
TERMS = 32
EPS = 1e-6
STEP = 0.5
SHIFT = 6.0
RADIUS = 6.0
HALO = 6
NX, NY, NZ = 4, 4, 8
PLANE = NX * NY
SLABS = PLANE + 2 * HALO
CHUNKS = 2
GROUP = 4
OFFSETS = (
    (2, 2), (2, 1), (1, 2), (2, 3), (3, 2), (1, 1), (3, 3), (1, 3), (3, 1),
    (2, 0), (0, 2), (1, 0), (0, 1), (3, 0), (0, 3),
)


def lanczos_weights(moments):
    first_norm = jnp.sqrt(moments[0] + EPS)
    inverse = 1.0 / first_norm
    sig = [value * inverse for value in moments]
    coef = [inverse]
    sig_prev, coef_prev, beta_prev = None, None, None
    alphas, betas, basis = [], [], []
    for j in range(ITERS):
        count = 2 * ITERS - 1 - j
        shifted = [0.5 * RADIUS * (sig[l + 1] + sig[abs(l - 1)]) for l in range(count)]
        alpha = coef[0] * (SHIFT * sig[0] + shifted[0])
        for k in range(1, j + 1):
            alpha = alpha + coef[k] * (SHIFT * sig[k] + shifted[k])
        alpha = jnp.clip(alpha, 0.0, 12.0)
        alphas.append(alpha)
        basis.append(coef)
        if j + 1 == ITERS:
            break
        rest = SHIFT - alpha
        r_sig = [shifted[l] + rest * sig[l] for l in range(count)]
        if j:
            r_sig = [r_sig[l] - beta_prev * sig_prev[l] for l in range(count)]
        r_coef = []
        for k in range(j + 2):
            terms = []
            if k >= 1:
                terms.append((RADIUS if k == 1 else 0.5 * RADIUS) * coef[k - 1])
            if k + 1 <= j:
                terms.append(0.5 * RADIUS * coef[k + 1])
            if k <= j:
                terms.append(rest * coef[k])
            if j and k < j:
                terms.append(-(beta_prev * coef_prev[k]))
            total = terms[0]
            for term in terms[1:]:
                total = total + term
            r_coef.append(total)
        square = r_coef[0] * r_sig[0]
        for k in range(1, j + 2):
            square = square + r_coef[k] * r_sig[k]
        beta = jnp.sqrt(jnp.clip(square, 0.0, 36.5) + EPS)
        betas.append(beta)
        scale = 1.0 / beta
        sig_prev, coef_prev, beta_prev = sig, coef, beta
        sig = [jnp.clip(value * scale, -first_norm, first_norm) for value in r_sig]
        coef = [value * scale for value in r_coef]
    zero = jnp.zeros_like(first_norm)
    term = [zero + 1.0] + [zero] * (ITERS - 1)
    sums = [list(term), [zero] * ITERS]
    for order in range(1, TERMS):
        factor = STEP / order if order % 2 == 0 else -STEP / order
        applied = []
        for i in range(ITERS):
            value = alphas[i] * term[i]
            if i + 1 < ITERS:
                value = value + betas[i] * term[i + 1]
            if i:
                value = value + betas[i - 1] * term[i - 1]
            applied.append(factor * value)
        term = applied
        sums[order % 2] = [a + b for a, b in zip(sums[order % 2], term)]
    weights = []
    for part in range(2):
        row = []
        for k in range(ITERS):
            total = sums[part][k] * basis[k][k]
            for j in range(k + 1, ITERS):
                total = total + sums[part][j] * basis[j][k]
            row.append(first_norm * total)
        weights.append(row)
    return weights


def kernel(psi_hbm, pot_hbm, out, psi, pot, snd, own_pot, pots, centre, u0, u1, u2, u3, u4, u5, crossed_z, matrix, partial, outs, back, mixed, gram, *sems):
    us = (u1, u2, u3, u4, u5)
    (psi_in, pot_in, pot_send, pot_recv, pot_halo_send, pot_halo_recv, in_send, in_recv, halo_send, halo_recv,
     gram_send, gram_recv, out_send, out_recv) = sems
    z, y, x, st = (lax.axis_index(name) for name in ("dom_0", "dom_1", "dom_2", "st"))
    me = y * NX + x
    lane = lax.broadcasted_iota(jnp.int32, (8, 128), 1)
    sub = lax.broadcasted_iota(jnp.int32, (8, 128), 0)

    def at(offset):
        to_y = lax.rem(y + offset[0], NY)
        to_x = lax.rem(x + offset[1], NX)
        return to_y * NX + to_x, (z, to_y, to_x, st)

    barrier = pltpu.get_barrier_semaphore()
    for offset in OFFSETS:
        pl.semaphore_signal(barrier, inc=1, device_id=at(offset)[1], device_id_type=MESH)
    for dz in range(1, NZ):
        pl.semaphore_signal(barrier, inc=1, device_id=(lax.rem(z + dz, NZ), y, x, st), device_id_type=MESH)

    load = pltpu.make_async_copy(psi_hbm, psi, psi_in)
    load.start()
    load_pot = pltpu.make_async_copy(pot_hbm, pot, pot_in)
    load_pot.start()

    from_lane = lax.broadcasted_iota(jnp.int32, (128, 128), 0)
    to_lane = lax.broadcasted_iota(jnp.int32, (128, 128), 1)
    apart = (from_lane - to_lane) & 63
    together = (from_lane & 64) == (to_lane & 64)
    along_z = jnp.where((apart == 1) | (apart == 63), 16.0, jnp.where((apart == 2) | (apart == 62), -1.0, 0.0))
    along_z = jnp.where(together, along_z, 0.0)
    swapped = jnp.where((from_lane ^ 64) == to_lane, 1.0, 0.0)
    for piece in range(2):
        matrix[128 * piece : 128 * piece + 128, 0:128] = along_z.astype(jnp.bfloat16)
        matrix[128 * piece : 128 * piece + 128, 128:256] = swapped.astype(jnp.bfloat16)

    load_pot.wait()
    for j in range(2):
        tile = jnp.concatenate([pot[0:4, j, :], pot[4:8, j, :]], axis=1)
        own_pot[4 * j : 4 * j + 4, :] = tile
    pots[HALO + me] = own_pot[...]

    wide = lax.broadcasted_iota(jnp.int32, (128, 128), 1)
    low = lax.rem(wide, 8) < 4

    def to_peers(chunk):
        for j in range(2):
            for i in range(4):
                re = jnp.concatenate([psi[0, i, j], psi[0, i + 4, j]], axis=0)
                im = jnp.concatenate([psi[1, i, j], psi[1, i + 4, j]], axis=0)
                if chunk == 0:
                    both = jnp.where(low, re, pltpu.roll(im, 4, 1))
                else:
                    both = jnp.where(low, pltpu.roll(re, 124, 1), im)
                snd[chunk, :, j, i] = both.T.reshape(PLANE, 8, 128)

    def send_in(chunk):
        for number, offset in enumerate(OFFSETS):
            peer, where = at(offset)
            pltpu.make_async_remote_copy(
                src_ref=snd.at[chunk, peer], dst_ref=u0.at[chunk, HALO + me],
                send_sem=in_send.at[chunk], recv_sem=in_recv.at[chunk, me],
                device_id=where, device_id_type=MESH,
            ).start()

    load.wait()
    to_peers(0)
    pl.semaphore_wait(barrier, len(OFFSETS) + NZ - 1)
    for number, offset in enumerate(OFFSETS):
        peer, where = at(offset)
        pltpu.make_async_remote_copy(
            src_ref=own_pot, dst_ref=pots.at[HALO + me],
            send_sem=pot_send, recv_sem=pot_recv,
            device_id=where, device_id_type=MESH,
        ).start()
    send_in(0)
    to_peers(1)
    send_in(1)
    for chunk in range(CHUNKS):
        u0[chunk, HALO + me] = snd[chunk, me]

    has_low, has_high = z > 0, z < NZ - 1
    below, above = (jnp.maximum(z - 1, 0), y, x, st), (jnp.minimum(z + 1, NZ - 1), y, x, st)

    @pl.when(jnp.logical_not(has_low))
    def _():
        for chunk in range(CHUNKS):
            u0[chunk, 0:HALO] = jnp.zeros((HALO,) + u0.shape[2:], jnp.float32)
        pots[0:HALO] = jnp.zeros((HALO, 8, 128), jnp.float32)

    @pl.when(jnp.logical_not(has_high))
    def _():
        for chunk in range(CHUNKS):
            u0[chunk, HALO + PLANE : SLABS] = jnp.zeros((HALO,) + u0.shape[2:], jnp.float32)
        pots[HALO + PLANE : SLABS] = jnp.zeros((HALO, 8, 128), jnp.float32)

    def wait_recv(ref, sem):
        pltpu.make_async_remote_copy(
            src_ref=ref, dst_ref=ref, send_sem=sem, recv_sem=sem,
            device_id=(z, y, x, st), device_id_type=MESH,
        ).wait_recv()

    def wait_send(ref, sem):
        pltpu.make_async_remote_copy(
            src_ref=ref, dst_ref=ref, send_sem=sem, recv_sem=sem,
            device_id=(z, y, x, st), device_id_type=MESH,
        ).wait_send()

    def halo_copy(chunk, slot, up):
        source = PLANE + slot if up else HALO + slot
        target = slot if up else HALO + PLANE + slot
        return pltpu.make_async_remote_copy(
            src_ref=u0.at[chunk, source], dst_ref=u0.at[chunk, target],
            send_sem=halo_send.at[chunk, int(up)], recv_sem=halo_recv.at[chunk, int(up)],
            device_id=above if up else below, device_id_type=MESH,
        )

    def pot_halo_copy(up):
        source = PLANE if up else HALO
        target = 0 if up else HALO + PLANE
        return pltpu.make_async_remote_copy(
            src_ref=pots.at[pl.ds(source, HALO)], dst_ref=pots.at[pl.ds(target, HALO)],
            send_sem=pot_halo_send.at[int(up)], recv_sem=pot_halo_recv.at[int(up)],
            device_id=above if up else below, device_id_type=MESH,
        )

    def forward(chunk):
        for p in range(PLANE):
            @pl.when(me != p)
            def _():
                wait_recv(u0.at[chunk, HALO + p], in_recv.at[chunk, p])
            if p < HALO:
                @pl.when(has_low)
                def _():
                    halo_copy(chunk, p, False).start()
            if p >= PLANE - HALO:
                @pl.when(has_high)
                def _():
                    halo_copy(chunk, p - PLANE + HALO, True).start()

    wait_recv(pots.at[pl.ds(0, PLANE - 1)], pot_recv)

    @pl.when(has_low)
    def _():
        pot_halo_copy(False).start()

    @pl.when(has_high)
    def _():
        pot_halo_copy(True).start()

    low_mask = jnp.where(has_low, 1.0, 0.0)
    high_mask = jnp.where(has_high, 1.0, 0.0)

    def set_centre(first, count):
        scaled = (2.0 / RADIUS) * pots[first : first + count] + (3.75 - SHIFT) * (2.0 / RADIUS)
        centre[first : first + count] = scaled

    set_centre(HALO, PLANE)
    far_w = (1.0 / 24.0) * (2.0 / RADIUS)

    def source(k):
        return us[k - 1] if k else u0

    def cross(chunk, k, first, count):
        value = source(k)[chunk, first : first + count].reshape(count * 64, 128)
        top = value.astype(jnp.bfloat16)
        rest = (value - top.astype(jnp.float32)).astype(jnp.bfloat16)
        crossed_z[first * 64 : (first + count) * 64, :] = jnp.dot(
            jnp.concatenate([top, rest], axis=1), matrix[...], preferred_element_type=jnp.float32
        )

    def apply(chunk, k, b, mask):
        u = source(k)
        rows = [[u[chunk, b + s, j, i] for i in range(4)] for s in (-1, 0, 1) for j in range(2)]
        values, results = [], []
        for j in range(2):
            row = rows[2 + j]
            start = b * 64 + j * 32
            swap = [crossed_z[start + 8 * i : start + 8 * i + 8, 128:256] for i in range(4)]
            ring = [swap[2], swap[3]] + row + [swap[0], swap[1]]
            for i in range(4):
                v = row[i]
                near = (ring[i + 1] + ring[i + 3]) + (rows[1 + j][i] + rows[3 + j][i])
                far = (ring[i] + ring[i + 4]) + (rows[j][i] + rows[4 + j][i])
                total = (16.0 * near - far) + crossed_z[start + 8 * i : start + 8 * i + 8, 0:128]
                new = centre[b, pl.ds(4 * j + i, 1), :] * v - far_w * total
                if k == 0:
                    new = 0.5 * new
                else:
                    new = new - source(k - 1)[chunk, b, j, i]
                if mask is not None:
                    new = new * mask
                values.append(v)
                results.append(new)
                if k + 1 < ITERS:
                    us[k][chunk, b, j, i] = new
        return values, results

    def tree(values):
        while len(values) > 1:
            values = [values[i] + values[i + 1] for i in range(0, len(values) - 1, 2)] + (
                [values[-1]] if len(values) % 2 else []
            )
        return values[0]

    zero = jnp.zeros((8, 128), jnp.float32)

    def run(chunk, k, ranges, sums):
        groups = []
        for first, last in ranges:
            groups += [(start, min(GROUP, last - start)) for start in range(first, last, GROUP)]
        cross(chunk, k, *groups[0])
        for number, (start, count) in enumerate(groups):
            if number + 1 < len(groups):
                cross(chunk, k, *groups[number + 1])
            for b in range(start, start + count):
                mine = HALO <= b < HALO + PLANE
                mask = None if mine else (low_mask if b < HALO else high_mask)
                values, results = apply(chunk, k, b, mask)
                if mine:
                    sums = (
                        sums[0] + tree([v * v for v in values]),
                        sums[1] + tree([v * r for v, r in zip(values, results)]),
                    )
        return sums

    def inner_range(k):
        return HALO + 1 + k, HALO + PLANE - 1 - k

    def inner(chunk, carry):
        forward(chunk)
        for k in range(ITERS):
            sums = run(chunk, k, [inner_range(k)], (zero, zero))
            for odd in range(2):
                partial[chunk, 2 * k + odd] = sums[odd]
        return carry

    def outer(chunk):
        tile = zero
        for k in range(ITERS):
            first, last = inner_range(k)
            sums = (partial[chunk, 2 * k], partial[chunk, 2 * k + 1])
            sums = run(chunk, k, [(1 + k, first), (last, SLABS - 1 - k)], sums)
            for odd in range(2):
                total = jnp.sum(sums[odd], axis=1, keepdims=True)
                tile = jnp.where(lane == 2 * k + odd, total, tile)
        return tile

    def send_gram(chunk):
        for dz in range(1, NZ):
            pltpu.make_async_remote_copy(
                src_ref=gram.at[chunk, z], dst_ref=gram.at[chunk, z],
                send_sem=gram_send.at[chunk], recv_sem=gram_recv.at[chunk],
                device_id=(lax.rem(z + dz, NZ), y, x, st), device_id_type=MESH,
            ).start()

    def advance(chunk, carry):
        @pl.when(has_low)
        def _():
            wait_recv(u0.at[chunk, pl.ds(0, HALO)], halo_recv.at[chunk, 1])

        @pl.when(has_high)
        def _():
            wait_recv(u0.at[chunk, pl.ds(0, HALO)], halo_recv.at[chunk, 0])
        gram[chunk, z] = outer(chunk)
        send_gram(chunk)
        return carry

    lax.fori_loop(0, CHUNKS, inner, 0)

    @pl.when(has_low)
    def _():
        pot_halo_copy(True).wait_recv()

    @pl.when(has_high)
    def _():
        pot_halo_copy(False).wait_recv()

    set_centre(0, HALO)
    set_centre(HALO + PLANE, HALO)
    lax.fori_loop(0, CHUNKS, advance, 0)

    wait_send(pots.at[pl.ds(0, PLANE - 1)], pot_send)
    for chunk in range(CHUNKS):
        wait_send(snd.at[chunk, pl.ds(0, PLANE - 1)], in_send.at[chunk])

    @pl.when(has_low)
    def _():
        pot_halo_copy(False).wait_send()
        for chunk in range(CHUNKS):
            wait_send(u0.at[chunk, pl.ds(0, HALO)], halo_send.at[chunk, 0])

    @pl.when(has_high)
    def _():
        pot_halo_copy(True).wait_send()
        for chunk in range(CHUNKS):
            wait_send(u0.at[chunk, pl.ds(0, HALO)], halo_send.at[chunk, 1])

    def finish(chunk):
        wait_recv(gram.at[chunk, pl.ds(0, NZ - 1)], gram_recv.at[chunk])
        total = tree([gram[chunk, p] for p in range(NZ)])
        total = total + pltpu.roll(total, 4, 0)
        raw = [jnp.broadcast_to(total[:, l : l + 1], (8, 128)) for l in range(2 * ITERS)]
        moments = raw[:2] + [2.0 * raw[l] - raw[l % 2] for l in range(2, 2 * ITERS)]
        real, imag = lanczos_weights(moments)
        imag = [jnp.where(sub < 4, value, -value) for value in imag]

        def combine(q, put):
            for j in range(2):
                for i in range(4):
                    v = u0[chunk, HALO + q, j, i]
                    straight, crossed = real[0] * v, imag[0] * v
                    for k in range(1, ITERS):
                        v = us[k - 1][chunk, HALO + q, j, i]
                        straight = straight + real[k] * v
                        crossed = crossed + imag[k] * v
                    put(j, i, straight + pltpu.roll(crossed, 4, 0))

        def send_out(offset):
            peer, where = at(offset)
            pltpu.make_async_remote_copy(
                src_ref=outs.at[chunk, peer], dst_ref=back.at[chunk, me],
                send_sem=out_send.at[chunk], recv_sem=out_recv.at[chunk],
                device_id=where, device_id_type=MESH,
            ).start()

        for number, offset in enumerate(OFFSETS):
            peer = at(offset)[0]

            def put(j, i, value):
                outs[chunk, peer, j, i] = value

            combine(peer, put)
            if number:
                send_out(OFFSETS[number - 1])

        def keep(j, i, value):
            back[chunk, me, j, i] = value

        combine(me, keep)
        send_out(OFFSETS[-1])

    for chunk in range(CHUNKS):
        finish(chunk)

    for chunk in range(CHUNKS):
        wait_recv(back.at[chunk, pl.ds(0, PLANE - 1)], out_recv.at[chunk])
        for j in range(2):
            for i in range(4):
                cells = back[chunk, :, j, i].reshape(128, 128).T
                if chunk == 0:
                    mixed[j, i] = cells
                else:
                    first = mixed[j, i]
                    re = jnp.where(low, first, pltpu.roll(cells, 4, 1))
                    im = jnp.where(low, pltpu.roll(first, 124, 1), cells)
                    out[0, i, j] = re[0:64]
                    out[0, i + 4, j] = re[64:128]
                    out[1, i, j] = im[0:64]
                    out[1, i + 4, j] = im[64:128]

    for chunk in range(CHUNKS):
        wait_send(gram.at[chunk, pl.ds(0, NZ - 1)], gram_send.at[chunk])
        wait_send(outs.at[chunk, pl.ds(0, PLANE - 1)], out_send.at[chunk])


def on_device(psi, potential):
    parts, _, cx, by, nz, orbs = psi.shape
    dma = pltpu.SemaphoreType.DMA
    tiles = (2, 4, 8, 128)
    result = pl.pallas_call(
        kernel,
        out_shape=jax.ShapeDtypeStruct((parts, cx, by, nz, orbs), jnp.float32),
        in_specs=[pl.BlockSpec(memory_space=pltpu.HBM)] * 2,
        out_specs=pl.BlockSpec(memory_space=pltpu.VMEM),
        scratch_shapes=[
            pltpu.VMEM((parts, cx, by, nz, orbs), jnp.float32),
            pltpu.VMEM((cx, by, nz), jnp.float32),
            pltpu.VMEM((CHUNKS, PLANE) + tiles, jnp.float32),
            pltpu.VMEM((8, 128), jnp.float32),
            pltpu.VMEM((SLABS, 8, 128), jnp.float32),
            pltpu.VMEM((SLABS, 8, 128), jnp.float32),
            *[pltpu.VMEM((CHUNKS, SLABS) + tiles, jnp.float32)] * ITERS,
            pltpu.VMEM((SLABS * 64, 256), jnp.float32),
            pltpu.VMEM((256, 256), jnp.bfloat16),
            pltpu.VMEM((CHUNKS, 2 * ITERS, 8, 128), jnp.float32),
            pltpu.VMEM((CHUNKS, PLANE) + tiles, jnp.float32),
            pltpu.VMEM((CHUNKS, PLANE) + tiles, jnp.float32),
            pltpu.VMEM((2, 4, 128, 128), jnp.float32),
            pltpu.VMEM((CHUNKS, NZ, 8, 128), jnp.float32),
            dma, dma, dma, dma, dma((2,)), dma((2,)),
            dma((CHUNKS,)), dma((CHUNKS, PLANE)),
            dma((CHUNKS, 2)), dma((CHUNKS, 2)),
            dma((CHUNKS,)), dma((CHUNKS,)),
            dma((CHUNKS,)), dma((CHUNKS,)),
        ],
        compiler_params=pltpu.CompilerParams(
            collective_id=0, has_side_effects=True, vmem_limit_bytes=48000000
        ),
    )(psi.reshape(parts, cx, by, nz, orbs), potential.reshape(cx, by, nz))
    return result.reshape(psi.shape)


def solution(mesh):
    names = ("dom_0", "dom_1", "dom_2", "st")
    torus = Mesh(mesh.devices.reshape(NZ, NY, NX, mesh.shape["st"]), names)
    placed = (P(None, names[:3], None, None, None, "st"), P(names[:3], None, None, None))
    return jax.shard_map(
        on_device,
        mesh=torus,
        in_specs=placed,
        out_specs=P(None, names[:3], None, None, None, "st"),
        check_vma=False,
    )
```

```python
import jax
import jax.numpy as jnp
from jax import lax
from jax.experimental import pallas as pl
from jax.experimental.pallas import tpu as pltpu
from jax.sharding import Mesh
from jax.sharding import PartitionSpec as P

MESH = pl.DeviceIdType.MESH
ITERS = 6
TERMS = 32
EPS = 1e-6
STEP = 0.5
SHIFT = 6.0
RADIUS = 6.0
HALO = 6
NX, NY, NZ = 4, 4, 8
PLANE = NX * NY
SLABS = PLANE + 2 * HALO
CHUNKS = 4
ORBS = 2
GROUP = 8
OFFSETS = (
    (2, 2), (2, 1), (1, 2), (2, 3), (3, 2), (1, 1), (3, 3), (1, 3), (3, 1),
    (2, 0), (0, 2), (1, 0), (0, 1), (3, 0), (0, 3),
)


def lanczos_weights(moments):
    first_norm = jnp.sqrt(moments[0] + EPS)
    inverse = 1.0 / first_norm
    sig = [value * inverse for value in moments]
    coef = [inverse]
    sig_prev, coef_prev, beta_prev = None, None, None
    alphas, betas, basis = [], [], []
    for j in range(ITERS):
        count = 2 * ITERS - 1 - j
        shifted = [0.5 * RADIUS * (sig[l + 1] + sig[abs(l - 1)]) for l in range(count)]
        alpha = coef[0] * (SHIFT * sig[0] + shifted[0])
        for k in range(1, j + 1):
            alpha = alpha + coef[k] * (SHIFT * sig[k] + shifted[k])
        alpha = jnp.clip(alpha, 0.0, 12.0)
        alphas.append(alpha)
        basis.append(coef)
        if j + 1 == ITERS:
            break
        rest = SHIFT - alpha
        r_sig = [shifted[l] + rest * sig[l] for l in range(count)]
        if j:
            r_sig = [r_sig[l] - beta_prev * sig_prev[l] for l in range(count)]
        r_coef = []
        for k in range(j + 2):
            terms = []
            if k >= 1:
                terms.append((RADIUS if k == 1 else 0.5 * RADIUS) * coef[k - 1])
            if k + 1 <= j:
                terms.append(0.5 * RADIUS * coef[k + 1])
            if k <= j:
                terms.append(rest * coef[k])
            if j and k < j:
                terms.append(-(beta_prev * coef_prev[k]))
            total = terms[0]
            for term in terms[1:]:
                total = total + term
            r_coef.append(total)
        square = r_coef[0] * r_sig[0]
        for k in range(1, j + 2):
            square = square + r_coef[k] * r_sig[k]
        beta = jnp.sqrt(jnp.clip(square, 0.0, 36.5) + EPS)
        betas.append(beta)
        scale = 1.0 / beta
        sig_prev, coef_prev, beta_prev = sig, coef, beta
        sig = [jnp.clip(value * scale, -first_norm, first_norm) for value in r_sig]
        coef = [value * scale for value in r_coef]
    zero = jnp.zeros_like(first_norm)
    term = [zero + 1.0] + [zero] * (ITERS - 1)
    sums = [list(term), [zero] * ITERS]
    for order in range(1, TERMS):
        factor = STEP / order if order % 2 == 0 else -STEP / order
        applied = []
        for i in range(ITERS):
            value = alphas[i] * term[i]
            if i + 1 < ITERS:
                value = value + betas[i] * term[i + 1]
            if i:
                value = value + betas[i - 1] * term[i - 1]
            applied.append(factor * value)
        term = applied
        sums[order % 2] = [a + b for a, b in zip(sums[order % 2], term)]
    weights = []
    for part in range(2):
        row = []
        for k in range(ITERS):
            total = sums[part][k] * basis[k][k]
            for j in range(k + 1, ITERS):
                total = total + sums[part][j] * basis[j][k]
            row.append(first_norm * total)
        weights.append(row)
    return weights


def kernel(psi_hbm, pot_hbm, out, psi, pot, snd, own_pot, pots, centre, u0, u1, u2, u3, u4, u5, crossed_z, matrix, partial, outs, back, mixed, gram, *sems):
    us = (u1, u2, u3, u4, u5)
    (psi_in, pot_in, pot_send, pot_recv, pot_halo_send, pot_halo_recv, in_send, in_recv, halo_send, halo_recv,
     gram_send, gram_recv, out_send, out_recv) = sems
    z, y, x, st = (lax.axis_index(name) for name in ("dom_0", "dom_1", "dom_2", "st"))
    me = y * NX + x
    lane = lax.broadcasted_iota(jnp.int32, (8, 128), 1)
    sub = lax.broadcasted_iota(jnp.int32, (8, 128), 0)

    def at(offset):
        to_y = lax.rem(y + offset[0], NY)
        to_x = lax.rem(x + offset[1], NX)
        return to_y * NX + to_x, (z, to_y, to_x, st)

    barrier = pltpu.get_barrier_semaphore()
    for offset in OFFSETS:
        pl.semaphore_signal(barrier, inc=1, device_id=at(offset)[1], device_id_type=MESH)
    for dz in range(1, NZ):
        pl.semaphore_signal(barrier, inc=1, device_id=(lax.rem(z + dz, NZ), y, x, st), device_id_type=MESH)

    load = pltpu.make_async_copy(psi_hbm, psi, psi_in)
    load.start()
    load_pot = pltpu.make_async_copy(pot_hbm, pot, pot_in)
    load_pot.start()

    from_lane = lax.broadcasted_iota(jnp.int32, (128, 128), 0)
    to_lane = lax.broadcasted_iota(jnp.int32, (128, 128), 1)
    apart = (from_lane - to_lane) & 63
    together = (from_lane & 64) == (to_lane & 64)
    along_z = jnp.where((apart == 1) | (apart == 63), 16.0, jnp.where((apart == 2) | (apart == 62), -1.0, 0.0))
    along_z = jnp.where(together, along_z, 0.0)
    swapped = jnp.where((from_lane ^ 64) == to_lane, 1.0, 0.0)
    for piece in range(2):
        matrix[128 * piece : 128 * piece + 128, 0:128] = along_z.astype(jnp.bfloat16)
        matrix[128 * piece : 128 * piece + 128, 128:256] = swapped.astype(jnp.bfloat16)

    load_pot.wait()
    for j in range(2):
        tile = jnp.concatenate([pot[0:4, j, :], pot[4:8, j, :]], axis=1)
        own_pot[4 * j : 4 * j + 4, :] = tile
    pots[HALO + me] = own_pot[...]

    wide = lax.broadcasted_iota(jnp.int32, (128, 128), 1)
    group = lax.shift_right_logical(wide, 1) & 3

    def merged(tiles, number):
        total = None
        for g in range(4):
            moved = tiles[g] if g == number else pltpu.roll(tiles[g], (2 * (g - number)) % 128, 1)
            total = moved if total is None else jnp.where(group == g, moved, total)
        return total

    def to_peers(chunks):
        for i in range(4):
            tiles = [
                jnp.concatenate([psi[part, i, j], psi[part, i + 4, j]], axis=0) for j in range(2) for part in range(2)
            ]
            for chunk in chunks:
                snd[chunk, :, i] = merged(tiles, chunk).T.reshape(PLANE, 8, 128)

    def rows(slab, count=1):
        return pl.ds(pl.multiple_of(8 * slab, 8), 8 * count)

    def send_in(chunk):
        for number, offset in enumerate(OFFSETS):
            peer, where = at(offset)
            pltpu.make_async_remote_copy(
                src_ref=snd.at[chunk, peer], dst_ref=u0.at[chunk, :, rows(HALO + me)],
                send_sem=in_send.at[chunk], recv_sem=in_recv.at[chunk, me],
                device_id=where, device_id_type=MESH,
            ).start()

    load.wait()
    to_peers((0,))
    pl.semaphore_wait(barrier, len(OFFSETS) + NZ - 1)
    for number, offset in enumerate(OFFSETS):
        peer, where = at(offset)
        pltpu.make_async_remote_copy(
            src_ref=own_pot, dst_ref=pots.at[HALO + me],
            send_sem=pot_send, recv_sem=pot_recv,
            device_id=where, device_id_type=MESH,
        ).start()
    send_in(0)
    for chunk in range(1, CHUNKS):
        to_peers((chunk,))
        send_in(chunk)
    for chunk in range(CHUNKS):
        u0[chunk, :, rows(HALO + me), :] = snd[chunk, me]

    has_low, has_high = z > 0, z < NZ - 1
    below, above = (jnp.maximum(z - 1, 0), y, x, st), (jnp.minimum(z + 1, NZ - 1), y, x, st)

    @pl.when(jnp.logical_not(has_low))
    def _():
        for chunk in range(CHUNKS):
            u0[chunk, :, 0 : 8 * HALO] = jnp.zeros((4, 8 * HALO, 128), jnp.float32)
        pots[0:HALO] = jnp.zeros((HALO, 8, 128), jnp.float32)

    @pl.when(jnp.logical_not(has_high))
    def _():
        for chunk in range(CHUNKS):
            u0[chunk, :, 8 * (HALO + PLANE) : 8 * SLABS] = jnp.zeros((4, 8 * HALO, 128), jnp.float32)
        pots[HALO + PLANE : SLABS] = jnp.zeros((HALO, 8, 128), jnp.float32)

    def wait_recv(ref, sem):
        pltpu.make_async_remote_copy(
            src_ref=ref, dst_ref=ref, send_sem=sem, recv_sem=sem,
            device_id=(z, y, x, st), device_id_type=MESH,
        ).wait_recv()

    def wait_send(ref, sem):
        pltpu.make_async_remote_copy(
            src_ref=ref, dst_ref=ref, send_sem=sem, recv_sem=sem,
            device_id=(z, y, x, st), device_id_type=MESH,
        ).wait_send()

    def halo_copy(chunk, p, up):
        target = p + HALO - PLANE if up else p + HALO + PLANE
        return pltpu.make_async_remote_copy(
            src_ref=u0.at[chunk, :, rows(HALO + p)], dst_ref=u0.at[chunk, :, rows(target)],
            send_sem=halo_send.at[chunk, int(up)], recv_sem=halo_recv.at[chunk, int(up)],
            device_id=above if up else below, device_id_type=MESH,
        )

    def pot_halo_copy(up):
        source = PLANE if up else HALO
        target = 0 if up else HALO + PLANE
        return pltpu.make_async_remote_copy(
            src_ref=pots.at[pl.ds(source, HALO)], dst_ref=pots.at[pl.ds(target, HALO)],
            send_sem=pot_halo_send.at[int(up)], recv_sem=pot_halo_recv.at[int(up)],
            device_id=above if up else below, device_id_type=MESH,
        )

    def pass_on(chunk, p):
        @pl.when(jnp.logical_and(has_low, p < HALO))
        def _():
            halo_copy(chunk, p, False).start()

        @pl.when(jnp.logical_and(has_high, p >= PLANE - HALO))
        def _():
            halo_copy(chunk, p, True).start()

    def forward(chunk):
        pass_on(chunk, me)
        for offset in OFFSETS:
            p = at((NY - offset[0], NX - offset[1]))[0]
            wait_recv(u0.at[chunk, :, rows(HALO)], in_recv.at[chunk, p])
            pass_on(chunk, p)

    wait_recv(pots.at[pl.ds(0, PLANE - 1)], pot_recv)

    @pl.when(has_low)
    def _():
        pot_halo_copy(False).start()

    @pl.when(has_high)
    def _():
        pot_halo_copy(True).start()

    low_mask = jnp.where(has_low, 1.0, 0.0)
    high_mask = jnp.where(has_high, 1.0, 0.0)

    def set_centre(first, count):
        for b in range(first, first + count):
            for i in range(4):
                tile = jnp.where(sub < 4, pots[b, i : i + 1, :], pots[b, 4 + i : 5 + i, :])
                centre[i, 8 * b : 8 * b + 8] = (2.0 / RADIUS) * tile + (3.75 - SHIFT) * (2.0 / RADIUS)

    set_centre(HALO, PLANE)
    far_w = (1.0 / 24.0) * (2.0 / RADIUS)

    def source(k):
        return us[k - 1] if k else u0

    def cross(k, chunk, first, count):
        value = source(k)[chunk, :, 8 * first : 8 * (first + count)].reshape(count * 32, 128)
        top = value.astype(jnp.bfloat16)
        rest = (value - top.astype(jnp.float32)).astype(jnp.bfloat16)
        product = jnp.dot(
            jnp.concatenate([top, rest], axis=1), matrix[...], preferred_element_type=jnp.float32
        )
        crossed_z[chunk % 2, :, 8 * first : 8 * (first + count)] = product.reshape(4, count * 8, 256)

    def apply(chunk, k, b, mask):
        u = source(k)
        here = slice(8 * b, 8 * b + 8)
        row = [u[chunk, i, here] for i in range(4)]
        swap = [crossed_z[chunk % 2, i, here, 128:256] for i in range(4)]
        ring = [swap[2], swap[3]] + row + [swap[0], swap[1]]
        results = []
        for i in range(4):
            y = [u[chunk, i, 8 * b + 4 * d : 8 * b + 4 * d + 8] for d in (-2, -1, 1, 2)]
            near = (ring[i + 1] + ring[i + 3]) + (y[1] + y[2])
            far = (ring[i] + ring[i + 4]) + (y[0] + y[3])
            total = (16.0 * near - far) + crossed_z[chunk % 2, i, here, 0:128]
            new = centre[i, here] * row[i] - far_w * total
            if k == 0:
                new = 0.5 * new
            else:
                new = new - source(k - 1)[chunk, i, here]
            if mask is not None:
                new = new * mask
            results.append(new)
            if k + 1 < ITERS:
                us[k][chunk, i, here] = new
        return row, results

    def tree(values):
        while len(values) > 1:
            values = [values[i] + values[i + 1] for i in range(0, len(values) - 1, 2)] + (
                [values[-1]] if len(values) % 2 else []
            )
        return values[0]

    zero = jnp.zeros((8, 128), jnp.float32)

    def inner_range(k):
        return HALO + 1 + k, HALO + PLANE - 1 - k

    def step(k, jobs):
        groups = []
        for chunk, ranges in jobs:
            for first, last in ranges:
                groups += [(chunk, start, min(GROUP, last - start)) for start in range(first, last, GROUP)]
        sums = {chunk: (zero, zero) for chunk, _ in jobs}
        cross(k, *groups[0])
        for number, (chunk, start, count) in enumerate(groups):
            if number + 1 < len(groups):
                cross(k, *groups[number + 1])
            for b in range(start, start + count):
                mine = HALO <= b < HALO + PLANE
                mask = None if mine else (low_mask if b < HALO else high_mask)
                values, results = apply(chunk, k, b, mask)
                if mine:
                    same, next_ = sums[chunk]
                    sums[chunk] = (
                        same + tree([v * v for v in values]),
                        next_ + tree([v * r for v, r in zip(values, results)]),
                    )
        return sums

    def advance(inner, outer):
        tile = zero
        for k in range(ITERS):
            first, last = inner_range(k)
            jobs = []
            if outer is not None:
                jobs.append((outer, [(1 + k, first), (last, SLABS - 1 - k)]))
            if inner is not None:
                jobs.append((inner, [(first, last)]))
            sums = step(k, jobs)
            for odd in range(2):
                if inner is not None:
                    partial[inner, 2 * k + odd] = sums[inner][odd]
                if outer is not None:
                    total = sums[outer][odd] + partial[outer, 2 * k + odd]
                    total = jnp.sum(total, axis=1, keepdims=True)
                    tile = jnp.where(lane == 2 * k + odd, total, tile)
        return tile

    def send_gram(chunk):
        for dz in range(1, NZ):
            pltpu.make_async_remote_copy(
                src_ref=gram.at[chunk, z], dst_ref=gram.at[chunk, z],
                send_sem=gram_send.at[chunk], recv_sem=gram_recv.at[chunk],
                device_id=(lax.rem(z + dz, NZ), y, x, st), device_id_type=MESH,
            ).start()

    def wait_halo(chunk):
        @pl.when(has_low)
        def _():
            wait_recv(u0.at[chunk, :, rows(0, HALO)], halo_recv.at[chunk, 1])

        @pl.when(has_high)
        def _():
            wait_recv(u0.at[chunk, :, rows(0, HALO)], halo_recv.at[chunk, 0])

    def finish(chunk):
        wait_recv(gram.at[chunk, pl.ds(0, NZ - 1)], gram_recv.at[chunk])
        total = tree([gram[chunk, p] for p in range(NZ)])
        total = total + pltpu.roll(total, 4, 0)
        total = total + pltpu.roll(total, 2, 0)
        raw = [jnp.broadcast_to(total[:, l : l + 1], (8, 128)) for l in range(2 * ITERS)]
        moments = raw[:2] + [2.0 * raw[l] - raw[l % 2] for l in range(2, 2 * ITERS)]
        real, imag = lanczos_weights(moments)
        real_rows = (sub & 2) == 0
        imag = [jnp.where(real_rows, value, -value) for value in imag]

        def combine(q, put):
            for i in range(4):
                v = u0[chunk, i, rows(HALO + q), :]
                straight, crossed = real[0] * v, imag[0] * v
                for k in range(1, ITERS):
                    v = us[k - 1][chunk, i, rows(HALO + q), :]
                    straight = straight + real[k] * v
                    crossed = crossed + imag[k] * v
                put(i, straight + jnp.where(real_rows, pltpu.roll(crossed, 6, 0), pltpu.roll(crossed, 2, 0)))

        def send_out(offset):
            peer, where = at(offset)
            pltpu.make_async_remote_copy(
                src_ref=outs.at[chunk, peer], dst_ref=back.at[chunk, me],
                send_sem=out_send.at[chunk], recv_sem=out_recv.at[chunk],
                device_id=where, device_id_type=MESH,
            ).start()

        for number, offset in enumerate(OFFSETS):
            peer = at(offset)[0]

            def put(i, value):
                outs[chunk, peer, i] = value

            combine(peer, put)
            if number:
                send_out(OFFSETS[number - 1])

        def keep(i, value):
            back[chunk, me, i] = value

        combine(me, keep)
        send_out(OFFSETS[-1])

    forward(0)
    advance(0, None)
    forward(1)

    @pl.when(has_low)
    def _():
        pot_halo_copy(True).wait_recv()

    @pl.when(has_high)
    def _():
        pot_halo_copy(False).wait_recv()

    set_centre(0, HALO)
    set_centre(HALO + PLANE, HALO)
    for chunk in range(CHUNKS):
        if 1 <= chunk < CHUNKS - 1:
            forward(chunk + 1)
        wait_halo(chunk)
        gram[chunk, z] = advance(chunk + 1 if chunk + 1 < CHUNKS else None, chunk)
        send_gram(chunk)
        if chunk == CHUNKS - 2:
            finish(0)
    for chunk in range(1, CHUNKS):
        finish(chunk)

    wait_send(pots.at[pl.ds(0, PLANE - 1)], pot_send)
    for chunk in range(CHUNKS):
        wait_send(snd.at[chunk, pl.ds(0, PLANE - 1)], in_send.at[chunk])
        wait_send(gram.at[chunk, pl.ds(0, NZ - 1)], gram_send.at[chunk])

    @pl.when(has_low)
    def _():
        pot_halo_copy(False).wait_send()
        for chunk in range(CHUNKS):
            wait_send(u0.at[chunk, :, rows(0, HALO)], halo_send.at[chunk, 0])

    @pl.when(has_high)
    def _():
        pot_halo_copy(True).wait_send()
        for chunk in range(CHUNKS):
            wait_send(u0.at[chunk, :, rows(0, HALO)], halo_send.at[chunk, 1])

    for chunk in range(CHUNKS):
        wait_recv(back.at[chunk, pl.ds(0, PLANE - 1)], out_recv.at[chunk])
        for i in range(4):
            tile = back[chunk, :, i].reshape(128, 128).T
            for g in range(4):
                moved = tile if g == chunk else pltpu.roll(tile, (2 * (chunk - g)) % 128, 1)
                whole = moved if chunk == 0 else jnp.where(group == chunk, moved, mixed[i, g])
                if chunk + 1 < CHUNKS:
                    mixed[i, g] = whole
                else:
                    out[g % 2, i, g // 2] = whole[0:64]
                    out[g % 2, i + 4, g // 2] = whole[64:128]
    for chunk in range(CHUNKS):
        wait_send(outs.at[chunk, pl.ds(0, PLANE - 1)], out_send.at[chunk])


def on_device(psi, potential):
    parts, _, cx, by, nz, orbs = psi.shape
    dma = pltpu.SemaphoreType.DMA
    tiles = (4, 8, 128)
    result = pl.pallas_call(
        kernel,
        out_shape=jax.ShapeDtypeStruct((parts, cx, by, nz, orbs), jnp.float32),
        in_specs=[pl.BlockSpec(memory_space=pl.ANY)] * 2,
        out_specs=pl.BlockSpec(memory_space=pltpu.VMEM),
        scratch_shapes=[
            pltpu.VMEM((parts, cx, by, nz, orbs), jnp.float32),
            pltpu.VMEM((cx, by, nz), jnp.float32),
            pltpu.VMEM((CHUNKS, PLANE) + tiles, jnp.float32),
            pltpu.VMEM((8, 128), jnp.float32),
            pltpu.VMEM((SLABS, 8, 128), jnp.float32),
            pltpu.VMEM((4, 8 * SLABS, 128), jnp.float32),
            *[pltpu.VMEM((CHUNKS, 4, 8 * SLABS, 128), jnp.float32)] * ITERS,
            pltpu.VMEM((2, 4, 8 * SLABS, 256), jnp.float32),
            pltpu.VMEM((256, 256), jnp.bfloat16),
            pltpu.VMEM((CHUNKS, 2 * ITERS, 8, 128), jnp.float32),
            pltpu.VMEM((CHUNKS, PLANE) + tiles, jnp.float32),
            pltpu.VMEM((CHUNKS, PLANE) + tiles, jnp.float32),
            pltpu.VMEM((4, 4, 128, 128), jnp.float32),
            pltpu.VMEM((CHUNKS, NZ, 8, 128), jnp.float32),
            dma, dma, dma, dma, dma((2,)), dma((2,)),
            dma((CHUNKS,)), dma((CHUNKS, PLANE)),
            dma((CHUNKS, 2)), dma((CHUNKS, 2)),
            dma((CHUNKS,)), dma((CHUNKS,)),
            dma((CHUNKS,)), dma((CHUNKS,)),
        ],
        compiler_params=pltpu.CompilerParams(
            collective_id=0, has_side_effects=True, vmem_limit_bytes=55500000
        ),
    )(psi.reshape(parts, cx, by, nz, orbs), potential.reshape(cx, by, nz))
    return result.reshape(psi.shape)


def solution(mesh):
    names = ("dom_0", "dom_1", "dom_2", "st")
    torus = Mesh(mesh.devices.reshape(NZ, NY, NX, mesh.shape["st"]), names)
    placed = (P(None, names[:3], None, None, None, "st"), P(names[:3], None, None, None))
    return jax.shard_map(
        on_device,
        mesh=torus,
        in_specs=placed,
        out_specs=P(None, names[:3], None, None, None, "st"),
        check_vma=False,
    )
```

```python
import jax
import jax.numpy as jnp
from jax import lax
from jax.experimental import pallas as pl
from jax.experimental.pallas import tpu as pltpu
from jax.sharding import Mesh
from jax.sharding import PartitionSpec as P

MESH = pl.DeviceIdType.MESH
ITERS = 6
TERMS = 32
EPS = 1e-6
STEP = 0.5
SHIFT = 6.0
RADIUS = 6.0
HALO = 6
NX, NY, NZ = 4, 4, 8
PLANE = NX * NY
SLABS = PLANE + 2 * HALO
PAIR = 2
CHUNKS = 4
ORBS = 2
GROUP = 4
OFFSETS = (
    (2, 2), (2, 1), (1, 2), (2, 3), (3, 2), (1, 1), (3, 3), (1, 3), (3, 1),
    (2, 0), (0, 2), (1, 0), (0, 1), (3, 0), (0, 3),
)


def lanczos_weights(moments):
    first_norm = jnp.sqrt(moments[0] + EPS)
    inverse = 1.0 / first_norm
    sig = [value * inverse for value in moments]
    coef = [inverse]
    sig_prev, coef_prev, beta_prev = None, None, None
    alphas, betas, basis = [], [], []
    for j in range(ITERS):
        count = 2 * ITERS - 1 - j
        shifted = [0.5 * RADIUS * (sig[l + 1] + sig[abs(l - 1)]) for l in range(count)]
        alpha = coef[0] * (SHIFT * sig[0] + shifted[0])
        for k in range(1, j + 1):
            alpha = alpha + coef[k] * (SHIFT * sig[k] + shifted[k])
        alpha = jnp.clip(alpha, 0.0, 12.0)
        alphas.append(alpha)
        basis.append(coef)
        if j + 1 == ITERS:
            break
        rest = SHIFT - alpha
        r_sig = [shifted[l] + rest * sig[l] for l in range(count)]
        if j:
            r_sig = [r_sig[l] - beta_prev * sig_prev[l] for l in range(count)]
        r_coef = []
        for k in range(j + 2):
            terms = []
            if k >= 1:
                terms.append((RADIUS if k == 1 else 0.5 * RADIUS) * coef[k - 1])
            if k + 1 <= j:
                terms.append(0.5 * RADIUS * coef[k + 1])
            if k <= j:
                terms.append(rest * coef[k])
            if j and k < j:
                terms.append(-(beta_prev * coef_prev[k]))
            total = terms[0]
            for term in terms[1:]:
                total = total + term
            r_coef.append(total)
        square = r_coef[0] * r_sig[0]
        for k in range(1, j + 2):
            square = square + r_coef[k] * r_sig[k]
        beta = jnp.sqrt(jnp.clip(square, 0.0, 36.5) + EPS)
        betas.append(beta)
        scale = 1.0 / beta
        sig_prev, coef_prev, beta_prev = sig, coef, beta
        sig = [jnp.clip(value * scale, -first_norm, first_norm) for value in r_sig]
        coef = [value * scale for value in r_coef]
    zero = jnp.zeros_like(first_norm)
    term = [zero + 1.0] + [zero] * (ITERS - 1)
    sums = [list(term), [zero] * ITERS]
    for order in range(1, TERMS):
        factor = STEP / order if order % 2 == 0 else -STEP / order
        applied = []
        for i in range(ITERS):
            value = alphas[i] * term[i]
            if i + 1 < ITERS:
                value = value + betas[i] * term[i + 1]
            if i:
                value = value + betas[i - 1] * term[i - 1]
            applied.append(factor * value)
        term = applied
        sums[order % 2] = [a + b for a, b in zip(sums[order % 2], term)]
    weights = []
    for part in range(2):
        row = []
        for k in range(ITERS):
            total = sums[part][k] * basis[k][k]
            for j in range(k + 1, ITERS):
                total = total + sums[part][j] * basis[j][k]
            row.append(first_norm * total)
        weights.append(row)
    return weights


def kernel(psi_hbm, pot_hbm, out, psi, pot, snd, own_pot, pots, centre, u0, u1, u2, u3, u4, u5, crossed_z, matrix, partial, outs, back, mixed, gram, *sems):
    us = (u1, u2, u3, u4, u5)
    (psi_in, pot_in, pot_send, pot_recv, pot_halo_send, pot_halo_recv, in_send, in_recv, halo_send, halo_recv,
     gram_send, gram_recv, out_send, out_recv) = sems
    z, y, x, st = (lax.axis_index(name) for name in ("dom_0", "dom_1", "dom_2", "st"))
    me = y * NX + x
    lane = lax.broadcasted_iota(jnp.int32, (8, 128), 1)
    sub = lax.broadcasted_iota(jnp.int32, (8, 128), 0)

    def at(offset):
        to_y = lax.rem(y + offset[0], NY)
        to_x = lax.rem(x + offset[1], NX)
        return to_y * NX + to_x, (z, to_y, to_x, st)

    barrier = pltpu.get_barrier_semaphore()
    for offset in OFFSETS:
        pl.semaphore_signal(barrier, inc=1, device_id=at(offset)[1], device_id_type=MESH)
    for dz in range(1, NZ):
        pl.semaphore_signal(barrier, inc=1, device_id=(lax.rem(z + dz, NZ), y, x, st), device_id_type=MESH)

    load = pltpu.make_async_copy(psi_hbm, psi, psi_in)
    load.start()
    load_pot = pltpu.make_async_copy(pot_hbm, pot, pot_in)
    load_pot.start()

    from_lane = lax.broadcasted_iota(jnp.int32, (128, 128), 0)
    to_lane = lax.broadcasted_iota(jnp.int32, (128, 128), 1)
    apart = (from_lane - to_lane) & 63
    together = (from_lane & 64) == (to_lane & 64)
    along_z = jnp.where((apart == 1) | (apart == 63), 16.0, jnp.where((apart == 2) | (apart == 62), -1.0, 0.0))
    along_z = jnp.where(together, along_z, 0.0)
    swapped = jnp.where((from_lane ^ 64) == to_lane, 1.0, 0.0)
    for piece in range(2):
        matrix[128 * piece : 128 * piece + 128, 0:128] = along_z.astype(jnp.bfloat16)
        matrix[128 * piece : 128 * piece + 128, 128:256] = swapped.astype(jnp.bfloat16)

    load_pot.wait()
    for j in range(2):
        tile = jnp.concatenate([pot[0:4, j, :], pot[4:8, j, :]], axis=1)
        own_pot[4 * j : 4 * j + 4, :] = tile
    pots[HALO + me] = own_pot[...]

    wide = lax.broadcasted_iota(jnp.int32, (128, 128), 1)
    group = lax.shift_right_logical(wide, 1) & 3

    def merged(tiles, number):
        total = None
        for g in range(4):
            moved = tiles[g] if g == number else pltpu.roll(tiles[g], (2 * (g - number)) % 128, 1)
            total = moved if total is None else jnp.where(group == g, moved, total)
        return total

    def to_peers(chunks):
        for i in range(4):
            tiles = [
                jnp.concatenate([psi[part, i, j], psi[part, i + 4, j]], axis=0) for j in range(2) for part in range(2)
            ]
            for chunk in chunks:
                snd[chunk, :, i] = merged(tiles, chunk).T.reshape(PLANE, 8, 128)

    def rows(slab, count=1):
        return pl.ds(8 * slab if isinstance(slab, int) else pl.multiple_of(8 * slab, 8), 8 * count)

    def send_in(chunk):
        for number, offset in enumerate(OFFSETS):
            peer, where = at(offset)
            pltpu.make_async_remote_copy(
                src_ref=snd.at[chunk, peer], dst_ref=u0.at[chunk, :, rows(HALO + me)],
                send_sem=in_send, recv_sem=in_recv.at[chunk, number // PAIR],
                device_id=where, device_id_type=MESH,
            ).start()

    load.wait()
    to_peers((0,))
    pl.semaphore_wait(barrier, len(OFFSETS) + NZ - 1)
    for number, offset in enumerate(OFFSETS):
        peer, where = at(offset)
        pltpu.make_async_remote_copy(
            src_ref=own_pot, dst_ref=pots.at[HALO + me],
            send_sem=pot_send, recv_sem=pot_recv,
            device_id=where, device_id_type=MESH,
        ).start()
    send_in(0)
    for chunk in range(1, CHUNKS):
        to_peers((chunk,))
        send_in(chunk)
    for chunk in range(CHUNKS):
        u0[chunk, :, rows(HALO + me), :] = snd[chunk, me]

    has_low, has_high = z > 0, z < NZ - 1
    below, above = (jnp.maximum(z - 1, 0), y, x, st), (jnp.minimum(z + 1, NZ - 1), y, x, st)

    @pl.when(jnp.logical_not(has_low))
    def _():
        for chunk in range(CHUNKS):
            u0[chunk, :, 0 : 8 * HALO] = jnp.zeros((4, 8 * HALO, 128), jnp.float32)
        pots[0:HALO] = jnp.zeros((HALO, 8, 128), jnp.float32)

    @pl.when(jnp.logical_not(has_high))
    def _():
        for chunk in range(CHUNKS):
            u0[chunk, :, 8 * (HALO + PLANE) : 8 * SLABS] = jnp.zeros((4, 8 * HALO, 128), jnp.float32)
        pots[HALO + PLANE : SLABS] = jnp.zeros((HALO, 8, 128), jnp.float32)

    def wait_recv(ref, sem):
        pltpu.make_async_remote_copy(
            src_ref=ref, dst_ref=ref, send_sem=sem, recv_sem=sem,
            device_id=(z, y, x, st), device_id_type=MESH,
        ).wait_recv()

    def wait_send(ref, sem):
        pltpu.make_async_remote_copy(
            src_ref=ref, dst_ref=ref, send_sem=sem, recv_sem=sem,
            device_id=(z, y, x, st), device_id_type=MESH,
        ).wait_send()

    def halo_copy(chunk, p, up):
        target = p + HALO - PLANE if up else p + HALO + PLANE
        return pltpu.make_async_remote_copy(
            src_ref=u0.at[chunk, :, rows(HALO + p)], dst_ref=u0.at[chunk, :, rows(target)],
            send_sem=halo_send.at[int(up)], recv_sem=halo_recv.at[chunk, int(up)],
            device_id=above if up else below, device_id_type=MESH,
        )

    def pot_halo_copy(up):
        source = PLANE if up else HALO
        target = 0 if up else HALO + PLANE
        return pltpu.make_async_remote_copy(
            src_ref=pots.at[pl.ds(source, HALO)], dst_ref=pots.at[pl.ds(target, HALO)],
            send_sem=pot_halo_send.at[int(up)], recv_sem=pot_halo_recv.at[int(up)],
            device_id=above if up else below, device_id_type=MESH,
        )

    def pass_on(chunk, p):
        @pl.when(jnp.logical_and(has_low, p < HALO))
        def _():
            halo_copy(chunk, p, False).start()

        @pl.when(jnp.logical_and(has_high, p >= PLANE - HALO))
        def _():
            halo_copy(chunk, p, True).start()

    def forward(chunk):
        pass_on(chunk, me)
        for first in range(0, len(OFFSETS), PAIR):
            some = OFFSETS[first : first + PAIR]
            wait_recv(u0.at[chunk, :, rows(HALO, len(some))], in_recv.at[chunk, first // PAIR])
            for offset in some:
                pass_on(chunk, at((NY - offset[0], NX - offset[1]))[0])

    wait_recv(pots.at[pl.ds(0, PLANE - 1)], pot_recv)

    @pl.when(has_low)
    def _():
        pot_halo_copy(False).start()

    @pl.when(has_high)
    def _():
        pot_halo_copy(True).start()

    low_mask = jnp.where(has_low, 1.0, 0.0)
    high_mask = jnp.where(has_high, 1.0, 0.0)

    def set_centre(first, count):
        for b in range(first, first + count):
            for i in range(4):
                tile = jnp.where(sub < 4, pots[b, i : i + 1, :], pots[b, 4 + i : 5 + i, :])
                centre[i, 8 * b : 8 * b + 8] = (2.0 / RADIUS) * tile + (3.75 - SHIFT) * (2.0 / RADIUS)

    set_centre(HALO, PLANE)
    far_w = (1.0 / 24.0) * (2.0 / RADIUS)

    def source(k):
        return us[k - 1] if k else u0

    def cross(k, chunk, first, count):
        value = source(k)[chunk, :, 8 * first : 8 * (first + count)].reshape(count * 32, 128)
        top = value.astype(jnp.bfloat16)
        rest = (value - top.astype(jnp.float32)).astype(jnp.bfloat16)
        product = jnp.dot(
            jnp.concatenate([top, rest], axis=1), matrix[...], preferred_element_type=jnp.float32
        )
        crossed_z[chunk % 2, :, 8 * first : 8 * (first + count)] = product.reshape(4, count * 8, 256)

    def apply(chunk, k, b, mask):
        u = source(k)
        here = slice(8 * b, 8 * b + 8)
        row = [u[chunk, i, here] for i in range(4)]
        swap = [crossed_z[chunk % 2, i, here, 128:256] for i in range(4)]
        ring = [swap[2], swap[3]] + row + [swap[0], swap[1]]
        results = []
        for i in range(4):
            y = [u[chunk, i, 8 * b + 4 * d : 8 * b + 4 * d + 8] for d in (-2, -1, 1, 2)]
            near = (ring[i + 1] + ring[i + 3]) + (y[1] + y[2])
            far = (ring[i] + ring[i + 4]) + (y[0] + y[3])
            total = (16.0 * near - far) + crossed_z[chunk % 2, i, here, 0:128]
            new = centre[i, here] * row[i] - far_w * total
            if k == 0:
                new = 0.5 * new
            else:
                new = new - source(k - 1)[chunk, i, here]
            if mask is not None:
                new = new * mask
            results.append(new)
            if k + 1 < ITERS:
                us[k][chunk, i, here] = new
        return row, results

    def tree(values):
        while len(values) > 1:
            values = [values[i] + values[i + 1] for i in range(0, len(values) - 1, 2)] + (
                [values[-1]] if len(values) % 2 else []
            )
        return values[0]

    zero = jnp.zeros((8, 128), jnp.float32)

    def inner_range(k):
        return HALO + 1 + k, HALO + PLANE - 1 - k

    def step(k, jobs):
        groups = []
        for chunk, ranges in jobs:
            for first, last in ranges:
                groups += [(chunk, start, min(GROUP, last - start)) for start in range(first, last, GROUP)]
        sums = {chunk: (zero, zero) for chunk, _ in jobs}
        cross(k, *groups[0])
        for number, (chunk, start, count) in enumerate(groups):
            if number + 1 < len(groups):
                cross(k, *groups[number + 1])
            for b in range(start, start + count):
                mine = HALO <= b < HALO + PLANE
                mask = None if mine else (low_mask if b < HALO else high_mask)
                values, results = apply(chunk, k, b, mask)
                if mine:
                    same, next_ = sums[chunk]
                    sums[chunk] = (
                        same + tree([v * v for v in values]),
                        next_ + tree([v * r for v, r in zip(values, results)]),
                    )
        return sums

    def advance(inner, outer):
        tile = zero
        for k in range(ITERS):
            first, last = inner_range(k)
            jobs = []
            if outer is not None:
                jobs.append((outer, [(1 + k, first), (last, SLABS - 1 - k)]))
            if inner is not None:
                jobs.append((inner, [(first, last)]))
            sums = step(k, jobs)
            for odd in range(2):
                if inner is not None:
                    partial[inner, 2 * k + odd] = sums[inner][odd]
                if outer is not None:
                    total = sums[outer][odd] + partial[outer, 2 * k + odd]
                    total = jnp.sum(total, axis=1, keepdims=True)
                    tile = jnp.where(lane == 2 * k + odd, total, tile)
        return tile

    def send_gram(chunk):
        for dz in range(1, NZ):
            pltpu.make_async_remote_copy(
                src_ref=gram.at[chunk, z], dst_ref=gram.at[chunk, z],
                send_sem=gram_send, recv_sem=gram_recv.at[chunk],
                device_id=(lax.rem(z + dz, NZ), y, x, st), device_id_type=MESH,
            ).start()

    def wait_halo(chunk):
        @pl.when(has_low)
        def _():
            wait_recv(u0.at[chunk, :, rows(0, HALO)], halo_recv.at[chunk, 1])

        @pl.when(has_high)
        def _():
            wait_recv(u0.at[chunk, :, rows(0, HALO)], halo_recv.at[chunk, 0])

    def finish(chunk):
        wait_recv(gram.at[chunk, pl.ds(0, NZ - 1)], gram_recv.at[chunk])
        total = tree([gram[chunk, p] for p in range(NZ)])
        total = total + pltpu.roll(total, 4, 0)
        total = total + pltpu.roll(total, 2, 0)
        raw = [jnp.broadcast_to(total[:, l : l + 1], (8, 128)) for l in range(2 * ITERS)]
        moments = raw[:2] + [2.0 * raw[l] - raw[l % 2] for l in range(2, 2 * ITERS)]
        real, imag = lanczos_weights(moments)
        real_rows = (sub & 2) == 0
        imag = [jnp.where(real_rows, value, -value) for value in imag]

        def combine(q, put):
            for i in range(4):
                v = u0[chunk, i, rows(HALO + q), :]
                straight, crossed = real[0] * v, imag[0] * v
                for k in range(1, ITERS):
                    v = us[k - 1][chunk, i, rows(HALO + q), :]
                    straight = straight + real[k] * v
                    crossed = crossed + imag[k] * v
                put(i, straight + jnp.where(real_rows, pltpu.roll(crossed, 6, 0), pltpu.roll(crossed, 2, 0)))

        def send_out(offset):
            peer, where = at(offset)
            pltpu.make_async_remote_copy(
                src_ref=outs.at[chunk, peer], dst_ref=back.at[chunk, me],
                send_sem=out_send, recv_sem=out_recv.at[chunk],
                device_id=where, device_id_type=MESH,
            ).start()

        for number, offset in enumerate(OFFSETS):
            peer = at(offset)[0]

            def put(i, value):
                outs[chunk, peer, i] = value

            combine(peer, put)
            if number:
                send_out(OFFSETS[number - 1])

        def keep(i, value):
            back[chunk, me, i] = value

        combine(me, keep)
        send_out(OFFSETS[-1])

    forward(0)
    advance(0, None)
    forward(1)

    @pl.when(has_low)
    def _():
        pot_halo_copy(True).wait_recv()

    @pl.when(has_high)
    def _():
        pot_halo_copy(False).wait_recv()

    set_centre(0, HALO)
    set_centre(HALO + PLANE, HALO)
    def close(chunk, inner):
        wait_halo(chunk)
        gram[chunk, z] = advance(inner, chunk)
        send_gram(chunk)

    close(0, 1)
    forward(2)
    close(1, 2)
    forward(3)
    advance(3, None)
    close(2, None)
    finish(0)
    close(3, None)
    for chunk in range(1, CHUNKS):
        finish(chunk)

    wait_send(pots.at[pl.ds(0, PLANE - 1)], pot_send)
    wait_send(snd.at[:, pl.ds(0, PLANE - 1)], in_send)
    wait_send(gram.at[:, pl.ds(0, NZ - 1)], gram_send)

    @pl.when(has_low)
    def _():
        pot_halo_copy(False).wait_send()
        wait_send(u0.at[:, :, rows(0, HALO)], halo_send.at[0])

    @pl.when(has_high)
    def _():
        pot_halo_copy(True).wait_send()
        wait_send(u0.at[:, :, rows(0, HALO)], halo_send.at[1])

    for chunk in range(CHUNKS):
        wait_recv(back.at[chunk, pl.ds(0, PLANE - 1)], out_recv.at[chunk])
        for i in range(4):
            tile = back[chunk, :, i].reshape(128, 128).T
            for g in range(4):
                moved = tile if g == chunk else pltpu.roll(tile, (2 * (chunk - g)) % 128, 1)
                whole = moved if chunk == 0 else jnp.where(group == chunk, moved, mixed[i, g])
                if chunk + 1 < CHUNKS:
                    mixed[i, g] = whole
                else:
                    out[g % 2, i, g // 2] = whole[0:64]
                    out[g % 2, i + 4, g // 2] = whole[64:128]
    wait_send(outs.at[:, pl.ds(0, PLANE - 1)], out_send)


def on_device(psi, potential):
    parts, _, cx, by, nz, orbs = psi.shape
    dma = pltpu.SemaphoreType.DMA
    tiles = (4, 8, 128)
    result = pl.pallas_call(
        kernel,
        out_shape=jax.ShapeDtypeStruct((parts, cx, by, nz, orbs), jnp.float32),
        in_specs=[pl.BlockSpec(memory_space=pl.ANY)] * 2,
        out_specs=pl.BlockSpec(memory_space=pltpu.VMEM),
        scratch_shapes=[
            pltpu.VMEM((parts, cx, by, nz, orbs), jnp.float32),
            pltpu.VMEM((cx, by, nz), jnp.float32),
            pltpu.VMEM((CHUNKS, PLANE) + tiles, jnp.float32),
            pltpu.VMEM((8, 128), jnp.float32),
            pltpu.VMEM((SLABS, 8, 128), jnp.float32),
            pltpu.VMEM((4, 8 * SLABS, 128), jnp.float32),
            *[pltpu.VMEM((CHUNKS, 4, 8 * SLABS, 128), jnp.float32)] * ITERS,
            pltpu.VMEM((2, 4, 8 * SLABS, 256), jnp.float32),
            pltpu.VMEM((256, 256), jnp.bfloat16),
            pltpu.VMEM((CHUNKS, 2 * ITERS, 8, 128), jnp.float32),
            pltpu.VMEM((CHUNKS, PLANE) + tiles, jnp.float32),
            pltpu.VMEM((CHUNKS, PLANE) + tiles, jnp.float32),
            pltpu.VMEM((4, 4, 128, 128), jnp.float32),
            pltpu.VMEM((CHUNKS, NZ, 8, 128), jnp.float32),
            dma, dma, dma, dma, dma((2,)), dma((2,)),
            dma, dma((CHUNKS, -(-len(OFFSETS) // PAIR))),
            dma((2,)), dma((CHUNKS, 2)),
            dma, dma((CHUNKS,)),
            dma, dma((CHUNKS,)),
        ],
        compiler_params=pltpu.CompilerParams(
            collective_id=0, has_side_effects=True, vmem_limit_bytes=55500000
        ),
    )(psi.reshape(parts, cx, by, nz, orbs), potential.reshape(cx, by, nz))
    return result.reshape(psi.shape)


def solution(mesh):
    names = ("dom_0", "dom_1", "dom_2", "st")
    torus = Mesh(mesh.devices.reshape(NZ, NY, NX, mesh.shape["st"]), names)
    placed = (P(None, names[:3], None, None, None, "st"), P(names[:3], None, None, None))
    return jax.shard_map(
        on_device,
        mesh=torus,
        in_specs=placed,
        out_specs=P(None, names[:3], None, None, None, "st"),
        check_vma=False,
    )
```
